32 devices in a mesh: row: 8 (over y, x, core), col: 4 (over z).
Axes of the slice: x: 2, y: 2, z: 4, core: 2. Of those that a mesh axis runs over, the one named last changes fastest.
Arguments:
- density: float32 [256, 256, 256], P('row', 'col'), may hold values from -5 to 5
- green_octant: float32 [256, 256, 256], P('row', 'col'), may hold values from 0 to 0.25
Outputs:
- potential: float32 [256, 256, 256], P('row', 'col')
The draws below stay inside these ranges and needn't reach their ends.
All inputs are finite; a program needn't handle non-finite values.
Results may differ from the reference program's by a relative error of at most 0.000092.
Values sent between devices are 32-bit elements; how exact they have to be, the bound alone decides.
A program may use at most 192 MiB of HBM per device.

```python
import math
import jax
import jax.numpy as jnp
from jax import lax

N = 256


def draw_density(key, part):
    noise = jax.random.normal(key, (N, N, N), jnp.float32)
    return jnp.clip(noise, -5.0, 5.0)


def draw_green_octant(key, part):
    coords = jnp.arange(N, dtype=jnp.float32)
    radius = jnp.sqrt(coords[:, None, None] * coords[:, None, None] + coords[None, :, None] * coords[None, :, None] + coords[None, None, :] * coords[None, None, :])
    factor = jnp.exp(jax.random.uniform(key, (N, N, N), jnp.float32, math.log(0.5), math.log(1.5)))
    return factor * jnp.exp(-radius / (N / 4.0)) / (4.0 * math.pi * jnp.maximum(radius, 0.5))


def setup_inputs(seed: int = 0) -> dict:
    streams_of = jax.random.split(jax.random.key(seed), 3)
    return {
        "density": draw_density(jax.random.fold_in(streams_of[2], 71), 0),
        "green_octant": draw_green_octant(jax.random.fold_in(streams_of[2], 71), 0),
    }


def cosine_table(extent, padded):
    positions = jnp.arange(extent, dtype=jnp.int32)[:, None]
    waves = jnp.arange(padded, dtype=jnp.int32)[None, :]
    phases = (positions * waves) % padded
    angles = phases.astype(jnp.float32) * jnp.float32(2.0 * 3.141592653589793 / padded)
    weights = jnp.where(positions == 0, jnp.float32(1.0), jnp.float32(2.0))
    return weights * jnp.cos(angles)


def reference(density, green_octant):
    padded = 2 * N
    table = cosine_table(N, padded)
    half_table = table[:, : N + 1]
    along_z = jnp.dot(green_octant.reshape(N * N, N), half_table, precision=lax.Precision.HIGHEST, preferred_element_type=jnp.float32).reshape(N, N, N + 1)
    along_y = jnp.einsum("ijk,jl->ilk", along_z, table, precision=lax.Precision.HIGHEST)
    kernel_hat = jnp.einsum("ijk,il->ljk", along_y, table, precision=lax.Precision.HIGHEST)
    density_hat = jnp.fft.rfftn(density, s=(padded, padded, padded))
    product = density_hat * kernel_hat
    whole = jnp.fft.irfftn(product, s=(padded, padded, padded))
    return whole[:N, :N, :N].astype(jnp.float32)
```

```python
import jax
import jax.numpy as jnp
import numpy as np
from jax import lax
from jax.experimental import pallas as pl
from jax.experimental.pallas import tpu as pltpu
from jax.sharding import PartitionSpec as P

F32 = jnp.float32
BF16 = jnp.bfloat16
VMEM_BYTES = 62 * 1024 * 1024
MESH = pl.DeviceIdType.MESH


def halves(table):
    table = np.asarray(table, np.float32)
    high = table.astype(BF16)
    low = (table - high.astype(np.float32)).astype(BF16)
    return jnp.asarray(np.stack([high, low]))


def split(value):
    high = value.astype(BF16)
    return high, (value - high.astype(F32)).astype(BF16)


def dot(a, b, dims=((1,), (0,))):
    return lax.dot_general(a, b, (dims, ((), ())), preferred_element_type=F32)


def dot3(left, right, dims=((1,), (0,))):
    return dot(left[0], right[0], dims) + (
        dot(left[0], right[1], dims) + dot(left[1], right[0], dims)
    )


def pair(ref):
    return ref[0], ref[1]


def fused_kernel(sizes, dens_ref, green_ref, f_ref, ft_ref, w_ref, wt_ref, fold_ref, out_ref,
                 dens_two, green_two, raw_out, raw_in, far_two, dsend, drecv, gsend, grecv,
                 bsend, brecv, ret_out, ret_in, total, raw_ssem, raw_rsem, d_ssem, d_rsem,
                 g_ssem, g_rsem, b_ssem, b_rsem, ret_ssem, ret_rsem):
    nrow, ncol, groups, per, width, each, blocks = sizes
    cells, extent = dens_ref.shape
    mid = extent // 2
    xl = groups * per
    hc = ncol // 2
    nsets = nrow * ncol
    team = nrow * hc
    chunks = extent // (team * each)
    row, col = lax.axis_index("row"), lax.axis_index("col")
    me = row * ncol + col
    half = lax.div(col, hc)
    away = 1 - half
    spot = col - half * hc
    rank = row * hc + spot
    relay_here = col == hc - 1 + half
    size = each * groups
    bgroups = groups // blocks

    def place(index):
        return lax.div(index, ncol), lax.rem(index, ncol)

    def greet(step, carry):
        pl.semaphore_signal(
            barrier, inc=1, device_id=place(lax.rem(me + step, nsets)), device_id_type=MESH
        )
        return carry

    barrier = pltpu.get_barrier_semaphore()
    lax.fori_loop(1, nsets, greet, 0)

    def remote(source, target, send_sem, recv_sem, device):
        return pltpu.make_async_remote_copy(
            src_ref=source,
            dst_ref=target,
            send_sem=send_sem,
            recv_sem=recv_sem,
            device_id=device,
            device_id_type=MESH,
        )

    def rows(ref, start, length):
        return ref.at[pl.ds(pl.multiple_of(start, 8), length), :]

    def wait(ref, length, sem):
        view = ref.at[pl.ds(0, length), :]
        pltpu.make_async_copy(view, view, sem).wait()

    def fold(g, carry):
        def pick(ref):
            return jnp.concatenate(
                [
                    ref[pl.ds(pl.multiple_of((h * groups + g) * width, width), width), :]
                    for h in range(per)
                ],
                axis=0,
            )

        start = pl.multiple_of(g * 128, 128)
        high, low = split(pick(dens_ref))
        dens_two[0, pl.ds(start, 128), :] = high
        dens_two[1, pl.ds(start, 128), :] = low
        raw_out[pl.ds(start, 128), :] = dot(high, fold_ref[away]) + dot(low, fold_ref[away])
        cell = lax.broadcasted_iota(jnp.int32, (128, extent), 0)
        z = lax.broadcasted_iota(jnp.int32, (128, extent), 1)
        lane_h = lax.div(cell, width)
        y = cell - lane_h * width + col * width
        x = lane_h * groups + g + row * xl
        weight = jnp.where(x == 0, 1.0, 2.0) * jnp.where(y == 0, 1.0, 2.0)
        weight = weight * jnp.where(z == 0, 1.0, 2.0) * (1.0 / (extent * extent * extent))
        high, low = split(pick(green_ref) * weight)
        green_two[0, pl.ds(start, 128), :] = high
        green_two[1, pl.ds(start, 128), :] = low
        return carry

    lax.fori_loop(0, groups, fold, 0)
    pl.semaphore_wait(barrier, nsets - 1)

    far_relay = (row, hc - 1 + away)
    brows = bgroups * 128
    for b in range(blocks):
        part = raw_out.at[pl.ds(b * brows, brows), :]
        remote(
            part, raw_in.at[spot, pl.ds(b * brows, brows), :], raw_ssem.at[b],
            raw_rsem.at[spot, b], far_relay,
        ).start()

    def transform(two, table, send, line):
        def tile(t, carry):
            start = pl.multiple_of(t * 256, 256)
            right = (two[0, pl.ds(start, 256), :], two[1, pl.ds(start, 256), :])
            result = dot3(table, right, ((1,), (1,)))
            for i in range(2):
                send[pl.ds(line * extent * groups + t * 2 + i, extent, stride=groups), :] = (
                    result[:, i * 128 : (i + 1) * 128]
                )
            return carry

        lax.fori_loop(0, cells // 256, tile, 0)

    w_here = (w_ref[half, 0], w_ref[half, 1])
    transform(dens_two, w_here, dsend, 0)

    def scatter_dens(chunk, line, source_set):
        def one(step, carry):
            target = lax.rem(rank + step, team)
            device = (lax.div(target, hc), lax.rem(target, hc) + half * hc)
            remote(
                rows(dsend, (line * extent + (chunk * team + target) * each) * groups, size),
                rows(drecv, (chunk * nsets + source_set) * size, size),
                d_ssem.at[chunk], d_rsem.at[chunk], device,
            ).start()
            return carry

        lax.fori_loop(1, team, one, 0)
        rows(drecv, (chunk * nsets + source_set) * size, size)[...] = rows(
            dsend, (line * extent + (chunk * team + rank) * each) * groups, size
        )[...]

    def scatter_own(chunk, carry):
        scatter_dens(chunk, 0, me)
        return carry

    lax.fori_loop(0, chunks, scatter_own, 0)

    transform(green_two, (ft_ref[0, 0:extent], ft_ref[1, 0:extent]), gsend, 0)

    def scatter_green(chunk, carry):
        def one(step, inner):
            target = lax.rem(me + step, nsets)
            r, c = place(target)
            owner = r * hc + lax.rem(c, hc)
            remote(
                rows(gsend, (chunk * team + owner) * size, size),
                rows(grecv, (chunk * nsets + me) * size, size),
                g_ssem.at[chunk], g_rsem.at[chunk], (r, c),
            ).start()
            return inner

        lax.fori_loop(1, nsets, one, 0)
        rows(grecv, (chunk * nsets + me) * size, size)[...] = rows(
            gsend, (chunk * team + rank) * size, size
        )[...]
        return carry

    lax.fori_loop(0, chunks, scatter_green, 0)

    @pl.when(relay_here)
    def _():
        for t in range(hc):
            for b in range(blocks):
                view = raw_in.at[t, pl.ds(b * brows, brows), :]
                pltpu.make_async_copy(view, view, raw_rsem.at[t, b]).wait()
                high, low = split(view[...])
                far_two[0, pl.ds(b * brows, brows), :] = high
                far_two[1, pl.ds(b * brows, brows), :] = low
            w_far = (w_ref[half, 0, :, 0:mid], w_ref[half, 1, :, 0:mid])
            transform(far_two, w_far, dsend, 1 + t)

            def scatter_far(chunk, carry):
                scatter_dens(chunk, 1 + t, row * ncol + away * hc + t)
                return carry

            lax.fori_loop(0, chunks, scatter_far, 0)

    def planes(chunk, carry):
        @pl.when(relay_here)
        def _():
            wait(drecv, (nsets - 1 - hc) * size, d_rsem.at[chunk])

        @pl.when(jnp.logical_not(relay_here))
        def _():
            wait(drecv, (nsets - 1) * size, d_rsem.at[chunk])

        wait(grecv, (nsets - 1) * size, g_rsem.at[chunk])

        def load(ref, slot):
            def piece(r, c):
                start = ((chunk * nsets + r * ncol + c) * each + slot) * groups
                return ref[pl.ds(start, groups), :]

            columns = [
                jnp.concatenate([piece(r, c) for r in range(nrow)], axis=0) for c in range(ncol)
            ]
            layers = [
                jnp.concatenate([v[:, h * width : (h + 1) * width] for v in columns], axis=1)
                for h in range(per)
            ]
            return jnp.concatenate(
                [v[r * groups : (r + 1) * groups] for r in range(nrow) for v in layers], axis=0
            )

        def one_slot(slot, inner):
            cosine = (f_ref[0, :, 0:extent], f_ref[1, :, 0:extent])
            green = dot3(split(load(grecv, slot)), cosine)
            green = dot3((ft_ref[0, 0:extent], ft_ref[1, 0:extent]), split(green))
            green = jnp.concatenate([green, green], axis=1)
            green = jnp.concatenate([green, green], axis=0)
            value = dot3(split(load(drecv, slot)), pair(f_ref))
            value = dot3(pair(ft_ref), split(value)) * green
            value = dot3(pair(f_ref), split(value))
            value = dot3(split(value), pair(ft_ref))
            for c in range(ncol):
                for r in range(nrow):
                    start = ((chunk * nsets + r * ncol + c) * each + slot) * groups
                    bsend[pl.ds(start, groups), :] = jnp.concatenate(
                        [
                            value[
                                r * xl + h * groups : r * xl + (h + 1) * groups,
                                c * width : (c + 1) * width,
                            ]
                            for h in range(per)
                        ],
                        axis=1,
                    )
            return inner

        lax.fori_loop(0, each, one_slot, 0)

        def back(step, inner):
            target = lax.rem(me + step, nsets)
            r, c = place(target)
            here = lax.div(c, hc) == half
            line = jnp.where(here, 0, 1 + lax.rem(c, hc))
            device = (r, jnp.where(here, c, hc - 1 + half))
            source = rows(bsend, (chunk * nsets + target) * size, size)
            sink = rows(brecv, (line * extent + (chunk * team + rank) * each) * groups, size)
            mine = jnp.logical_and(device[0] == row, device[1] == col)

            @pl.when(mine)
            def _():
                sink[...] = source[...]

            @pl.when(jnp.logical_not(mine))
            def _():
                remote(source, sink, b_ssem.at[chunk], b_rsem.at[chunk], device).start()

            return inner

        lax.fori_loop(0, nsets, back, 0)
        return carry

    lax.fori_loop(0, chunks, planes, 0)

    def settle(chunk, carry):
        @pl.when(relay_here)
        def _():
            wait(brecv, (1 + hc) * (team - 1) * size, b_rsem.at[chunk])

        @pl.when(jnp.logical_not(relay_here))
        def _():
            wait(brecv, (team - 1) * size, b_rsem.at[chunk])

        return carry

    lax.fori_loop(0, chunks, settle, 0)

    def lines(line, group):
        return split(brecv[pl.ds(line * extent * groups + group, extent, stride=groups), :])

    @pl.when(relay_here)
    def _():
        table = (wt_ref[half, 0, 0:mid, :], wt_ref[half, 1, 0:mid, :])

        def far_block(b, carry):
            for t in range(hc):
                def far_group(i, inner):
                    g = b * bgroups + i
                    start = pl.multiple_of(g * mid, 8)
                    ret_out[t, pl.ds(start, mid), :] = dot3(table, lines(1 + t, g))
                    return inner

                lax.fori_loop(0, bgroups, far_group, 0)
                start = pl.multiple_of(b * bgroups * mid, 8)
                remote(
                    ret_out.at[t, pl.ds(start, bgroups * mid), :],
                    ret_in.at[pl.ds(start, bgroups * mid), :],
                    ret_ssem.at[b], ret_rsem.at[b], (row, away * hc + t),
                ).start()
            return carry

        lax.fori_loop(0, blocks, far_block, 0)

    def near_group(g, carry):
        start = pl.multiple_of(g * extent, 8)
        total[pl.ds(start, extent), :] = dot3((wt_ref[half, 0], wt_ref[half, 1]), lines(0, g))
        return carry

    lax.fori_loop(0, groups, near_group, 0)

    def finish(b, carry):
        start = pl.multiple_of(b * bgroups * mid, 8)
        view = ret_in.at[pl.ds(start, bgroups * mid), :]
        pltpu.make_async_copy(view, view, ret_rsem.at[b]).wait()

        def one_group(i, inner):
            g = b * bgroups + i
            high, low = split(ret_in[pl.ds(pl.multiple_of(g * mid, 8), mid), :])
            value = dot(fold_ref[away], high) + dot(fold_ref[away], low)
            value = value + total[pl.ds(pl.multiple_of(g * extent, 8), extent), :]
            value = value.T
            for h in range(per):
                start = pl.multiple_of((h * groups + g) * width, width)
                out_ref[pl.ds(start, width), :] = value[h * width : (h + 1) * width]
            return inner

        lax.fori_loop(0, bgroups, one_group, 0)
        return carry

    lax.fori_loop(0, blocks, finish, 0)

    for b in range(blocks):
        view = raw_out.at[pl.ds(b * brows, brows), :]
        pltpu.make_async_copy(view, view, raw_ssem.at[b]).wait()

    def drain(chunk, carry):
        wait(grecv, (nsets - 1) * size, g_ssem.at[chunk])

        @pl.when(relay_here)
        def _():
            wait(dsend, (1 + hc) * (team - 1) * size, d_ssem.at[chunk])
            wait(bsend, (nsets - 1 - hc) * size, b_ssem.at[chunk])

        @pl.when(jnp.logical_not(relay_here))
        def _():
            wait(dsend, (team - 1) * size, d_ssem.at[chunk])
            wait(bsend, (nsets - 1) * size, b_ssem.at[chunk])

        return carry

    lax.fori_loop(0, chunks, drain, 0)

    @pl.when(relay_here)
    def _():
        for b in range(blocks):
            view = ret_in.at[pl.ds(0, hc * bgroups * mid), :]
            pltpu.make_async_copy(view, view, ret_ssem.at[b]).wait()


def make(mesh):
    nrow, ncol = mesh.shape["row"], mesh.shape["col"]

    def on_device(density, green_octant):
        xl, width, extent = density.shape
        per = 128 // width
        groups = xl // per
        cells = xl * width
        hc = ncol // 2
        team = nrow * hc
        slots = extent // team
        each = min(EACH, slots)
        chunks = slots // each
        blocks = min(4, groups)
        mid = extent // 2
        k = np.arange(extent)[:, None]
        n = np.arange(extent)[None, :]
        theta = np.pi / (2 * extent) * (((2 * k + 1) * n) % (4 * extent))
        both = np.concatenate([np.cos(theta), np.sin(theta)], axis=0)
        shifted = np.pi / (4 * extent) * (((2 * k + 1) * (2 * n + 1 - extent)) % (8 * extent))
        waves = np.stack([np.cos(shifted), np.sin(shifted)])
        flip = np.eye(extent)[:, :mid]
        fold = np.stack([flip + flip[::-1], flip - flip[::-1]])
        tables = (
            halves(both.T),
            halves(both),
            halves(waves).transpose(1, 0, 2, 3),
            halves(waves.transpose(0, 2, 1)).transpose(1, 0, 2, 3),
            jnp.asarray(fold.astype(np.float32).astype(BF16)),
        )
        operands = (
            density.reshape(cells, extent),
            green_octant.reshape(cells, extent),
        ) + tables
        sizes = (nrow, ncol, groups, per, width, each, blocks)
        lot = extent * groups
        dma = pltpu.SemaphoreType.DMA
        out = pl.pallas_call(
            lambda *refs: fused_kernel(sizes, *refs),
            in_specs=[pl.BlockSpec(memory_space=pltpu.VMEM)] * len(operands),
            out_specs=pl.BlockSpec(memory_space=pltpu.VMEM),
            out_shape=jax.ShapeDtypeStruct((cells, extent), F32),
            scratch_shapes=[
                pltpu.VMEM((2, cells, extent), BF16),
                pltpu.VMEM((2, cells, extent), BF16),
                pltpu.VMEM((cells, mid), F32),
                pltpu.VMEM((hc, cells, mid), F32),
                pltpu.VMEM((2, cells, mid), BF16),
                pltpu.VMEM(((1 + hc) * lot, 128), F32),
                pltpu.VMEM((2 * lot, 128), F32),
                pltpu.VMEM((lot, 128), F32),
                pltpu.VMEM((2 * lot, 128), F32),
                pltpu.VMEM((2 * lot, 128), F32),
                pltpu.VMEM(((1 + hc) * lot, 128), F32),
                pltpu.VMEM((hc, groups * mid, 128), F32),
                pltpu.VMEM((groups * mid, 128), F32),
                pltpu.VMEM((groups * extent, 128), F32),
                dma((blocks,)),
                dma((hc, blocks)),
                dma((chunks,)),
                dma((chunks,)),
                dma((chunks,)),
                dma((chunks,)),
                dma((chunks,)),
                dma((chunks,)),
                dma((blocks,)),
                dma((blocks,)),
            ],
            compiler_params=pltpu.CompilerParams(
                vmem_limit_bytes=VMEM_BYTES, collective_id=0, has_side_effects=True
            ),
            name="fused",
        )(*operands)
        return out.reshape(xl, width, extent)

    return on_device


EACH = 4


def solution(mesh):
    return jax.shard_map(
        make(mesh),
        mesh=mesh,
        in_specs=(P("row", "col", None), P("row", "col", None)),
        out_specs=P("row", "col", None),
        check_vma=False,
    )
```

```python
import jax
import jax.numpy as jnp
import numpy as np
from jax import lax
from jax.experimental import pallas as pl
from jax.experimental.pallas import tpu as pltpu
from jax.sharding import PartitionSpec as P

F32 = jnp.float32
BF16 = jnp.bfloat16
VMEM_BYTES = 62 * 1024 * 1024
MESH = pl.DeviceIdType.MESH


def halves(table):
    table = np.asarray(table, np.float32)
    high = table.astype(BF16)
    low = (table - high.astype(np.float32)).astype(BF16)
    return jnp.asarray(np.stack([high, low]))


def split(value):
    high = value.astype(BF16)
    return high, (value - high.astype(F32)).astype(BF16)


def dot(a, b, dims=((1,), (0,))):
    return lax.dot_general(a, b, (dims, ((), ())), preferred_element_type=F32)


def dot3(left, right, dims=((1,), (0,))):
    return dot(left[0], right[0], dims) + (
        dot(left[0], right[1], dims) + dot(left[1], right[0], dims)
    )


def pair(ref):
    return ref[0], ref[1]


def fused_kernel(sizes, dens_hbm, green_hbm, f_hbm, ft_hbm, w_hbm, wt_hbm, fold_hbm, out_hbm,
                 dens_in, green_in, f_ref, ft_ref, w_ref, wt_ref, fold_ref, out_ref,
                 dens_two, green_two, raw_out, raw_in, far_two, dsend, drecv, gsend, grecv,
                 bsend, brecv, ret_out, ret_in, total, in_sem, dens_sem, out_sem, raw_ssem,
                 raw_rsem, d_ssem, d_rsem, g_ssem, g_rsem, b_ssem, b_rsem, ret_ssem, ret_rsem, n_ssem, n_rsem):
    nrow, ncol, groups, per, width, each, blocks = sizes
    cells, extent = dens_in.shape
    mid = extent // 2
    xl = groups * per
    hc = ncol // 2
    nsets = nrow * ncol
    team = nrow * hc
    chunks = extent // (team * each)
    row, col = lax.axis_index("row"), lax.axis_index("col")
    me = row * ncol + col
    half = lax.div(col, hc)
    away = 1 - half
    spot = col - half * hc
    rank = row * hc + spot
    relay_here = col == hc - 1 + half
    size = each * groups
    bgroups = groups // blocks
    brows = bgroups * 128

    def place(index):
        return lax.div(index, ncol), lax.rem(index, ncol)

    def greet(step, carry):
        pl.semaphore_signal(
            barrier, inc=1, device_id=place(lax.rem(me + step, nsets)), device_id_type=MESH
        )
        return carry

    barrier = pltpu.get_barrier_semaphore()
    lax.fori_loop(1, nsets, greet, 0)

    def strip(ref, b, h):
        start = (h * groups + b * bgroups) * width
        return ref.at[pl.ds(start, bgroups * width), :]

    dens_copies = [
        [
            pltpu.make_async_copy(strip(dens_hbm, b, h), strip(dens_in, b, h), dens_sem.at[b, h])
            for h in range(per)
        ]
        for b in range(blocks)
    ]
    copies = [
        pltpu.make_async_copy(source, target, in_sem.at[i])
        for i, (source, target) in enumerate(
            (
                (fold_hbm, fold_ref),
                (w_hbm, w_ref),
                (green_hbm, green_in),
                (ft_hbm, ft_ref),
                (f_hbm, f_ref),
                (wt_hbm, wt_ref),
            )
        )
    ]
    copies[0].start()
    for b in range(blocks):
        for copy in dens_copies[b]:
            copy.start()
    for copy in copies[1:]:
        copy.start()

    def remote(source, target, send_sem, recv_sem, device):
        return pltpu.make_async_remote_copy(
            src_ref=source,
            dst_ref=target,
            send_sem=send_sem,
            recv_sem=recv_sem,
            device_id=device,
            device_id_type=MESH,
        )

    def rows(ref, start, length):
        return ref.at[pl.ds(pl.multiple_of(start, 8), length), :]

    def wait(ref, length, sem):
        view = ref.at[pl.ds(0, length), :]
        pltpu.make_async_copy(view, view, sem).wait()

    def pick(ref, g):
        return jnp.concatenate(
            [
                ref[pl.ds(pl.multiple_of((h * groups + g) * width, width), width), :]
                for h in range(per)
            ],
            axis=0,
        )

    def fold(g, carry):
        start = pl.multiple_of(g * 128, 128)
        high, low = split(pick(dens_in, g))
        dens_two[0, pl.ds(start, 128), :] = high
        dens_two[1, pl.ds(start, 128), :] = low
        raw_out[pl.ds(start, 128), :] = dot(high, fold_ref[away]) + dot(low, fold_ref[away])
        return carry

    copies[0].wait()
    for b in range(blocks):
        for copy in dens_copies[b]:
            copy.wait()
        lax.fori_loop(b * bgroups, (b + 1) * bgroups, fold, 0)
        if b == 0:
            pl.semaphore_wait(barrier, nsets - 1)
        remote(
            rows(raw_out, b * brows, brows), rows(raw_in.at[spot], b * brows, brows),
            raw_ssem.at[b], raw_rsem.at[spot, b], (row, hc - 1 + away),
        ).start()

    def transform(two, table, send, line):
        def tile(t, carry):
            start = pl.multiple_of(t * 256, 256)
            right = (two[0, pl.ds(start, 256), :], two[1, pl.ds(start, 256), :])
            result = dot3(table, right, ((1,), (1,)))
            for i in range(2):
                send[pl.ds(line * extent * groups + t * 2 + i, extent, stride=groups), :] = (
                    result[:, i * 128 : (i + 1) * 128]
                )
            return carry

        lax.fori_loop(0, cells // 256, tile, 0)

    copies[1].wait()
    transform(dens_two, (w_ref[half, 0], w_ref[half, 1]), dsend, 0)

    def scatter_dens(lines_sets):
        def one_chunk(chunk, outer):
            def one(step, carry):
                target = lax.rem(rank + step, team)
                device = (lax.div(target, hc), lax.rem(target, hc) + half * hc)
                for line, sets in lines_sets:
                    remote(
                        rows(
                            dsend, (line * extent + (chunk * team + target) * each) * groups, size
                        ),
                        rows(drecv, (chunk * nsets + sets) * size, size),
                        d_ssem.at[chunk], d_rsem.at[chunk], device,
                    ).start()
                return carry

            lax.fori_loop(1, team, one, 0)
            for line, sets in lines_sets:
                rows(drecv, (chunk * nsets + sets) * size, size)[...] = rows(
                    dsend, (line * extent + (chunk * team + rank) * each) * groups, size
                )[...]
            return outer

        lax.fori_loop(0, chunks, one_chunk, 0)

    scatter_dens([(0, me)])

    def weigh(g, carry):
        cell = lax.broadcasted_iota(jnp.int32, (128, extent), 0)
        z = lax.broadcasted_iota(jnp.int32, (128, extent), 1)
        lane_h = lax.div(cell, width)
        y = cell - lane_h * width + col * width
        x = lane_h * groups + g + row * xl
        weight = jnp.where(x == 0, 1.0, 2.0) * jnp.where(y == 0, 1.0, 2.0)
        weight = weight * jnp.where(z == 0, 1.0, 2.0) * (1.0 / (extent * extent * extent))
        start = pl.multiple_of(g * 128, 128)
        high, low = split(pick(green_in, g) * weight)
        green_two[0, pl.ds(start, 128), :] = high
        green_two[1, pl.ds(start, 128), :] = low
        return carry

    copies[2].wait()
    copies[3].wait()
    lax.fori_loop(0, groups, weigh, 0)
    transform(green_two, (ft_ref[0, 0:extent], ft_ref[1, 0:extent]), gsend, 0)

    def scatter_green(chunk, carry):
        def one(step, inner):
            target = lax.rem(me + step, nsets)
            r, c = place(target)
            owner = r * hc + lax.rem(c, hc)
            remote(
                rows(gsend, (chunk * team + owner) * size, size),
                rows(grecv, (chunk * nsets + me) * size, size),
                g_ssem.at[chunk], g_rsem.at[chunk], (r, c),
            ).start()
            return inner

        lax.fori_loop(1, nsets, one, 0)
        rows(grecv, (chunk * nsets + me) * size, size)[...] = rows(
            gsend, (chunk * team + rank) * size, size
        )[...]
        return carry

    lax.fori_loop(0, chunks, scatter_green, 0)
    copies[4].wait()
    copies[5].wait()

    @pl.when(relay_here)
    def _():
        for t in range(hc):
            for b in range(blocks):
                view = rows(raw_in.at[t], b * brows, brows)
                pltpu.make_async_copy(view, view, raw_rsem.at[t, b]).wait()
                high, low = split(view[...])
                far_two[0, pl.ds(b * brows, brows), :] = high
                far_two[1, pl.ds(b * brows, brows), :] = low
            w_far = (w_ref[half, 0, :, 0:mid], w_ref[half, 1, :, 0:mid])
            transform(far_two, w_far, dsend, 1 + t)
        scatter_dens([(1 + t, row * ncol + away * hc + t) for t in range(hc)])

    def planes(chunk, carry):
        @pl.when(relay_here)
        def _():
            wait(drecv, (nsets - 1 - hc) * size, d_rsem.at[chunk])

        @pl.when(jnp.logical_not(relay_here))
        def _():
            wait(drecv, (nsets - 1) * size, d_rsem.at[chunk])

        wait(grecv, (nsets - 1) * size, g_rsem.at[chunk])

        def load(ref, slot):
            def piece(r, c):
                start = ((chunk * nsets + r * ncol + c) * each + slot) * groups
                return ref[pl.ds(start, groups), :]

            columns = [
                jnp.concatenate([piece(r, c) for r in range(nrow)], axis=0) for c in range(ncol)
            ]
            layers = [
                jnp.concatenate([v[:, h * width : (h + 1) * width] for v in columns], axis=1)
                for h in range(per)
            ]
            return jnp.concatenate(
                [v[r * groups : (r + 1) * groups] for r in range(nrow) for v in layers], axis=0
            )

        def one_slot(slot, inner):
            cosine = (f_ref[0, :, 0:extent], f_ref[1, :, 0:extent])
            green = dot3(split(load(grecv, slot)), cosine)
            green = dot3((ft_ref[0, 0:extent], ft_ref[1, 0:extent]), split(green))
            green = jnp.concatenate([green, green], axis=1)
            green = jnp.concatenate([green, green], axis=0)
            value = dot3(split(load(drecv, slot)), pair(f_ref))
            value = dot3(pair(ft_ref), split(value)) * green
            value = dot3(pair(f_ref), split(value))
            value = dot3(split(value), pair(ft_ref))
            for c in range(ncol):
                for r in range(nrow):
                    start = ((chunk * nsets + r * ncol + c) * each + slot) * groups
                    bsend[pl.ds(start, groups), :] = jnp.concatenate(
                        [
                            value[
                                r * xl + h * groups : r * xl + (h + 1) * groups,
                                c * width : (c + 1) * width,
                            ]
                            for h in range(per)
                        ],
                        axis=1,
                    )
            return inner

        lax.fori_loop(0, each, one_slot, 0)

        def back(step, inner):
            r = lax.rem(row + step, nrow)
            mine = jnp.logical_and(relay_here, r == row)
            for t in range(hc):
                source = rows(bsend, (chunk * nsets + r * ncol + away * hc + t) * size, size)
                start = ((1 + t) * extent + (chunk * team + rank) * each) * groups
                sink = rows(brecv, start, size)

                @pl.when(mine)
                def _():
                    sink[...] = source[...]

                @pl.when(jnp.logical_not(mine))
                def _():
                    remote(
                        source, sink, b_ssem.at[chunk], b_rsem.at[chunk], (r, hc - 1 + half)
                    ).start()

            return inner

        lax.fori_loop(0, nrow, back, 0)
        return carry

    lax.fori_loop(0, chunks, planes, 0)

    def near_back(chunk, carry):
        sink = rows(brecv, (chunk * team + rank) * size, size)

        def one(step, inner):
            target = lax.rem(rank + step, team)
            r, c = lax.div(target, hc), lax.rem(target, hc) + half * hc
            source = rows(bsend, (chunk * nsets + r * ncol + c) * size, size)
            remote(source, sink, n_ssem.at[0], n_rsem.at[0], (r, c)).start()
            return inner

        lax.fori_loop(1, team, one, 0)
        sink[...] = rows(bsend, (chunk * nsets + me) * size, size)[...]
        return carry

    lax.fori_loop(0, chunks, near_back, 0)

    def lines(line, group):
        return split(brecv[pl.ds(line * extent * groups + group, extent, stride=groups), :])

    far_table = (wt_ref[half, 0, 0:mid, :], wt_ref[half, 1, 0:mid, :])

    @pl.when(relay_here)
    def _():
        def settle(chunk, carry):
            wait(brecv, hc * (team - 1) * size, b_rsem.at[chunk])
            return carry

        lax.fori_loop(0, chunks, settle, 0)

        def far_block(b, carry):
            for t in range(hc):
                def far_group(i, inner):
                    g = b * bgroups + i
                    start = pl.multiple_of(g * mid, 8)
                    ret_out[t, pl.ds(start, mid), :] = dot3(far_table, lines(1 + t, g))
                    return inner

                lax.fori_loop(0, bgroups, far_group, 0)
                remote(
                    rows(ret_out.at[t], b * bgroups * mid, bgroups * mid),
                    rows(ret_in, b * bgroups * mid, bgroups * mid),
                    ret_ssem.at[b], ret_rsem.at[b], (row, away * hc + t),
                ).start()
            return carry

        lax.fori_loop(0, blocks, far_block, 0)

    wait(brecv, (team - 1) * chunks * size, n_rsem.at[0])

    def near_group(g, carry):
        start = pl.multiple_of(g * extent, 8)
        total[pl.ds(start, extent), :] = dot3((wt_ref[half, 0], wt_ref[half, 1]), lines(0, g))
        return carry

    lax.fori_loop(0, groups, near_group, 0)

    out_copies = [
        [
            pltpu.make_async_copy(strip(out_ref, b, h), strip(out_hbm, b, h), out_sem.at[b, h])
            for h in range(per)
        ]
        for b in range(blocks)
    ]
    for b in range(blocks):
        view = rows(ret_in, b * bgroups * mid, bgroups * mid)
        pltpu.make_async_copy(view, view, ret_rsem.at[b]).wait()

        def one_group(g, inner):
            high, low = split(ret_in[pl.ds(pl.multiple_of(g * mid, 8), mid), :])
            value = dot(fold_ref[away], high) + dot(fold_ref[away], low)
            value = value + total[pl.ds(pl.multiple_of(g * extent, 8), extent), :]
            value = value.T
            for h in range(per):
                start = pl.multiple_of((h * groups + g) * width, width)
                out_ref[pl.ds(start, width), :] = value[h * width : (h + 1) * width]
            return inner

        lax.fori_loop(b * bgroups, (b + 1) * bgroups, one_group, 0)
        for copy in out_copies[b]:
            copy.start()

    for b in range(blocks):
        wait(raw_out, brows, raw_ssem.at[b])

    wait(brecv, (team - 1) * chunks * size, n_ssem.at[0])

    @pl.when(relay_here)
    def _():
        for b in range(blocks):
            wait(raw_out, hc * bgroups * mid, ret_ssem.at[b])

    def drain(chunk, carry):
        wait(grecv, (nsets - 1) * size, g_ssem.at[chunk])

        @pl.when(relay_here)
        def _():
            wait(dsend, (1 + hc) * (team - 1) * size, d_ssem.at[chunk])
            wait(bsend, hc * (nrow - 1) * size, b_ssem.at[chunk])

        @pl.when(jnp.logical_not(relay_here))
        def _():
            wait(dsend, (team - 1) * size, d_ssem.at[chunk])
            wait(bsend, hc * nrow * size, b_ssem.at[chunk])

        return carry

    lax.fori_loop(0, chunks, drain, 0)
    for b in range(blocks):
        for copy in out_copies[b]:
            copy.wait()


def make(mesh):
    nrow, ncol = mesh.shape["row"], mesh.shape["col"]

    def on_device(density, green_octant):
        xl, width, extent = density.shape
        per = 128 // width
        groups = xl // per
        cells = xl * width
        hc = ncol // 2
        team = nrow * hc
        slots = extent // team
        each = min(EACH, slots)
        chunks = slots // each
        blocks = min(BLOCKS, groups)
        mid = extent // 2
        k = np.arange(extent)[:, None]
        n = np.arange(extent)[None, :]
        theta = np.pi / (2 * extent) * (((2 * k + 1) * n) % (4 * extent))
        both = np.concatenate([np.cos(theta), np.sin(theta)], axis=0)
        shifted = np.pi / (4 * extent) * (((2 * k + 1) * (2 * n + 1 - extent)) % (8 * extent))
        waves = np.stack([np.cos(shifted), np.sin(shifted)])
        flip = np.eye(extent)[:, :mid]
        fold = np.stack([flip + flip[::-1], flip - flip[::-1]])
        tables = (
            halves(both.T),
            halves(both),
            halves(waves).transpose(1, 0, 2, 3),
            halves(waves.transpose(0, 2, 1)).transpose(1, 0, 2, 3),
            jnp.asarray(fold.astype(np.float32).astype(BF16)),
        )
        operands = (
            density.reshape(cells, extent),
            green_octant.reshape(cells, extent),
        ) + tables
        sizes = (nrow, ncol, groups, per, width, each, blocks)
        lot = extent * groups
        dma = pltpu.SemaphoreType.DMA
        any_space = pl.BlockSpec(memory_space=pl.ANY)
        out = pl.pallas_call(
            lambda *refs: fused_kernel(sizes, *refs),
            in_specs=[any_space] * len(operands),
            out_specs=any_space,
            out_shape=jax.ShapeDtypeStruct((cells, extent), F32),
            scratch_shapes=[pltpu.VMEM(v.shape, v.dtype) for v in operands]
            + [
                pltpu.VMEM((cells, extent), F32),
                pltpu.VMEM((2, cells, extent), BF16),
                pltpu.VMEM((2, cells, extent), BF16),
                pltpu.VMEM((cells, mid), F32),
                pltpu.VMEM((hc, cells, mid), F32),
                pltpu.VMEM((2, cells, mid), BF16),
                pltpu.VMEM(((1 + hc) * lot, 128), F32),
                pltpu.VMEM((2 * lot, 128), F32),
                pltpu.VMEM((lot, 128), F32),
                pltpu.VMEM((2 * lot, 128), F32),
                pltpu.VMEM((2 * lot, 128), F32),
                pltpu.VMEM(((1 + hc) * lot, 128), F32),
                pltpu.VMEM((hc, groups * mid, 128), F32),
                pltpu.VMEM((groups * mid, 128), F32),
                pltpu.VMEM((groups * extent, 128), F32),
                dma((6,)),
                dma((blocks, per)),
                dma((blocks, per)),
                dma((blocks,)),
                dma((hc, blocks)),
            ]
            + [dma((chunks,))] * 6
            + [dma((blocks,))] * 2
            + [dma((1,))] * 2,
            compiler_params=pltpu.CompilerParams(
                vmem_limit_bytes=VMEM_BYTES, collective_id=0, has_side_effects=True
            ),
            name="fused",
        )(*operands)
        return out.reshape(xl, width, extent)

    return on_device


EACH = 2
BLOCKS = 8


def solution(mesh):
    return jax.shard_map(
        make(mesh),
        mesh=mesh,
        in_specs=(P("row", "col", None), P("row", "col", None)),
        out_specs=P("row", "col", None),
        check_vma=False,
    )
```

```python
import jax
import jax.numpy as jnp
import numpy as np
from jax import lax
from jax.experimental import pallas as pl
from jax.experimental.pallas import tpu as pltpu
from jax.sharding import PartitionSpec as P

F32 = jnp.float32
BF16 = jnp.bfloat16
VMEM_BYTES = 62 * 1024 * 1024
MESH = pl.DeviceIdType.MESH


def halves(table):
    table = np.asarray(table, np.float32)
    high = table.astype(BF16)
    low = (table - high.astype(np.float32)).astype(BF16)
    return jnp.asarray(np.stack([high, low]))


def split(value):
    high = value.astype(BF16)
    return high, (value - high.astype(F32)).astype(BF16)


def dot(a, b, dims=((1,), (0,))):
    return lax.dot_general(a, b, (dims, ((), ())), preferred_element_type=F32)


def dot3(left, right, dims=((1,), (0,))):
    return dot(left[0], right[0], dims) + (
        dot(left[0], right[1], dims) + dot(left[1], right[0], dims)
    )


def pair(ref):
    return ref[0], ref[1]


def fused_kernel(sizes, dens_hbm, green_hbm, f_hbm, ft_hbm, w_hbm, wt_hbm, fold_hbm, out_hbm,
                 dens_in, green_in, f_ref, ft_ref, w_ref, wt_ref, fold_ref, out_ref,
                 dens_two, green_two, raw_out, raw_in, far_two, dsend, drecv, gsend, grecv,
                 bsend, brecv, ret_out, ret_in, total, in_sem, dens_sem, out_sem, raw_ssem,
                 raw_rsem, d_ssem, d_rsem, g_ssem, g_rsem, b_ssem, b_rsem, ret_ssem, ret_rsem, n_ssem, n_rsem,
                 o_rsem):
    nrow, ncol, groups, per, width, each, blocks = sizes
    cells, extent = dens_in.shape
    mid = extent // 2
    xl = groups * per
    hc = ncol // 2
    nsets = nrow * ncol
    team = nrow * hc
    chunks = extent // (team * each)
    row, col = lax.axis_index("row"), lax.axis_index("col")
    me = row * ncol + col
    half = lax.div(col, hc)
    away = 1 - half
    spot = col - half * hc
    rank = row * hc + spot
    relay_spot = (hc - 1) * away
    relay_here = spot == relay_spot
    outer = nrow * (hc - 1)
    size = each * groups
    bgroups = groups // blocks
    brows = bgroups * 128

    def place(index):
        return lax.div(index, ncol), lax.rem(index, ncol)

    def greet(step, carry):
        pl.semaphore_signal(
            barrier, inc=1, device_id=place(lax.rem(me + step, nsets)), device_id_type=MESH
        )
        return carry

    barrier = pltpu.get_barrier_semaphore()
    lax.fori_loop(1, nsets, greet, 0)

    def strip(ref, b, h):
        start = (h * groups + b * bgroups) * width
        return ref.at[pl.ds(start, bgroups * width), :]

    dens_copies = [
        [
            pltpu.make_async_copy(strip(dens_hbm, b, h), strip(dens_in, b, h), dens_sem.at[b, h])
            for h in range(per)
        ]
        for b in range(blocks)
    ]
    copies = [
        pltpu.make_async_copy(source, target, in_sem.at[i])
        for i, (source, target) in enumerate(
            (
                (fold_hbm, fold_ref),
                (w_hbm, w_ref),
                (green_hbm, green_in),
                (ft_hbm, ft_ref),
                (f_hbm, f_ref),
                (wt_hbm, wt_ref),
            )
        )
    ]
    copies[0].start()
    for b in range(blocks):
        for copy in dens_copies[b]:
            copy.start()
    for copy in copies[1:]:
        copy.start()

    def remote(source, target, send_sem, recv_sem, device):
        return pltpu.make_async_remote_copy(
            src_ref=source,
            dst_ref=target,
            send_sem=send_sem,
            recv_sem=recv_sem,
            device_id=device,
            device_id_type=MESH,
        )

    def rows(ref, start, length):
        return ref.at[pl.ds(pl.multiple_of(start, 8), length), :]

    def wait(ref, length, sem):
        view = ref.at[pl.ds(0, length), :]
        pltpu.make_async_copy(view, view, sem).wait()

    def pick(ref, g):
        return jnp.concatenate(
            [
                ref[pl.ds(pl.multiple_of((h * groups + g) * width, width), width), :]
                for h in range(per)
            ],
            axis=0,
        )

    def fold(g, carry):
        start = pl.multiple_of(g * 128, 128)
        high, low = split(pick(dens_in, g))
        dens_two[0, pl.ds(start, 128), :] = high
        dens_two[1, pl.ds(start, 128), :] = low
        raw_out[pl.ds(start, 128), :] = dot(high, fold_ref[away]) + dot(low, fold_ref[away])
        return carry

    copies[0].wait()
    for b in range(blocks):
        for copy in dens_copies[b]:
            copy.wait()
        lax.fori_loop(b * bgroups, (b + 1) * bgroups, fold, 0)
        if b == 0:
            pl.semaphore_wait(barrier, nsets - 1)
        remote(
            rows(raw_out, b * brows, brows), rows(raw_in.at[spot], b * brows, brows),
            raw_ssem.at[b], raw_rsem.at[spot, b], (row, hc - 1 + away),
        ).start()

    def transform(two, table, send, line):
        def tile(t, carry):
            start = pl.multiple_of(t * 256, 256)
            right = (two[0, pl.ds(start, 256), :], two[1, pl.ds(start, 256), :])
            result = dot3(table, right, ((1,), (1,)))
            for i in range(2):
                send[pl.ds(line * extent * groups + t * 2 + i, extent, stride=groups), :] = (
                    result[:, i * 128 : (i + 1) * 128]
                )
            return carry

        lax.fori_loop(0, cells // 256, tile, 0)

    copies[1].wait()
    transform(dens_two, (w_ref[half, 0], w_ref[half, 1]), dsend, 0)

    def scatter_dens(lines_sets):
        def one_chunk(chunk, outer):
            def one(step, carry):
                target = lax.rem(rank + step, team)
                device = (lax.div(target, hc), lax.rem(target, hc) + half * hc)
                for line, sets in lines_sets:
                    remote(
                        rows(
                            dsend, (line * extent + (chunk * team + target) * each) * groups, size
                        ),
                        rows(drecv, (chunk * nsets + sets) * size, size),
                        d_ssem.at[chunk], d_rsem.at[chunk], device,
                    ).start()
                return carry

            lax.fori_loop(1, team, one, 0)
            for line, sets in lines_sets:
                rows(drecv, (chunk * nsets + sets) * size, size)[...] = rows(
                    dsend, (line * extent + (chunk * team + rank) * each) * groups, size
                )[...]
            return outer

        lax.fori_loop(0, chunks, one_chunk, 0)

    scatter_dens([(0, me)])

    def weigh(g, carry):
        cell = lax.broadcasted_iota(jnp.int32, (128, extent), 0)
        z = lax.broadcasted_iota(jnp.int32, (128, extent), 1)
        lane_h = lax.div(cell, width)
        y = cell - lane_h * width + col * width
        x = lane_h * groups + g + row * xl
        weight = jnp.where(x == 0, 1.0, 2.0) * jnp.where(y == 0, 1.0, 2.0)
        weight = weight * jnp.where(z == 0, 1.0, 2.0) * (1.0 / (extent * extent * extent))
        start = pl.multiple_of(g * 128, 128)
        high, low = split(pick(green_in, g) * weight)
        green_two[0, pl.ds(start, 128), :] = high
        green_two[1, pl.ds(start, 128), :] = low
        return carry

    copies[2].wait()
    copies[3].wait()
    lax.fori_loop(0, groups, weigh, 0)
    transform(green_two, (ft_ref[0, 0:extent], ft_ref[1, 0:extent]), gsend, 0)

    def green_to(chunk, r, s, side, sem):
        remote(
            rows(gsend, (chunk * team + r * hc + s) * size, size),
            rows(grecv, (chunk * nsets + me) * size, size),
            g_ssem.at[chunk], sem.at[chunk], (r, s + side * hc),
        ).start()

    def green_inside(chunk, carry):
        def one(step, inner):
            target = lax.rem(rank + step, team)
            r, s = lax.div(target, hc), lax.rem(target, hc)
            via = jnp.logical_and(jnp.logical_not(relay_here), s == relay_spot)

            @pl.when(via)
            def _():
                green_to(chunk, r, s, half, o_rsem)

            @pl.when(jnp.logical_not(via))
            def _():
                green_to(chunk, r, s, half, g_rsem)

            return inner

        lax.fori_loop(1, team, one, 0)
        rows(grecv, (chunk * nsets + me) * size, size)[...] = rows(
            gsend, (chunk * team + rank) * size, size
        )[...]
        return carry

    def green_away(chunk, carry):
        def one(step, inner):
            target = lax.rem(rank + step, team)
            r, s = lax.div(target, hc), lax.rem(target, hc)

            @pl.when(jnp.logical_or(relay_here, s != relay_spot))
            def _():
                green_to(chunk, r, s, away, g_rsem)

            return inner

        lax.fori_loop(0, team, one, 0)
        return carry

    def hand_on(chunk):
        wait(grecv, outer * size, o_rsem.at[chunk])
        for i in range(hc - 1):
            s = i + lax.convert_element_type(relay_spot <= i, jnp.int32)

            def one(r, inner):
                block = rows(grecv, (chunk * nsets + r * ncol + half * hc + s) * size, size)
                remote(
                    block, block, g_ssem.at[chunk], g_rsem.at[chunk],
                    (row, away * hc + relay_spot),
                ).start()
                return inner

            lax.fori_loop(0, nrow, one, 0)

    def pace(chunk):
        @pl.when(jnp.logical_and(relay_here, chunk < chunks))
        def _():
            hand_on(chunk)

        @pl.when(jnp.logical_and(relay_here, chunk + LEAD < chunks))
        def _():
            green_away(chunk + LEAD, 0)

    lead = jnp.where(relay_here, min(LEAD, chunks), chunks)

    def green_first(chunk, carry):
        green_inside(chunk, 0)

        @pl.when(chunk < lead)
        def _():
            green_away(chunk, 0)

        return carry

    lax.fori_loop(0, chunks, green_first, 0)
    copies[4].wait()
    copies[5].wait()

    @pl.when(relay_here)
    def _():
        for t in range(hc):
            for b in range(blocks):
                view = rows(raw_in.at[t], b * brows, brows)
                pltpu.make_async_copy(view, view, raw_rsem.at[t, b]).wait()
                high, low = split(view[...])
                far_two[0, pl.ds(b * brows, brows), :] = high
                far_two[1, pl.ds(b * brows, brows), :] = low
            w_far = (w_ref[half, 0, :, 0:mid], w_ref[half, 1, :, 0:mid])
            transform(far_two, w_far, dsend, 1 + t)
        scatter_dens([(1 + t, row * ncol + away * hc + t) for t in range(hc)])

    pace(0)

    def planes(chunk, carry):
        pace(chunk + 1)

        @pl.when(relay_here)
        def _():
            wait(drecv, (nsets - 1 - hc) * size, d_rsem.at[chunk])
            wait(grecv, (nsets - 1 - outer) * size, g_rsem.at[chunk])

        @pl.when(jnp.logical_not(relay_here))
        def _():
            wait(drecv, (nsets - 1) * size, d_rsem.at[chunk])
            wait(grecv, (nsets - 1) * size, g_rsem.at[chunk])

        def load(ref, slot):
            def piece(r, c):
                start = ((chunk * nsets + r * ncol + c) * each + slot) * groups
                return ref[pl.ds(start, groups), :]

            columns = [
                jnp.concatenate([piece(r, c) for r in range(nrow)], axis=0) for c in range(ncol)
            ]
            layers = [
                jnp.concatenate([v[:, h * width : (h + 1) * width] for v in columns], axis=1)
                for h in range(per)
            ]
            return jnp.concatenate(
                [v[r * groups : (r + 1) * groups] for r in range(nrow) for v in layers], axis=0
            )

        def one_slot(slot, inner):
            cosine = (f_ref[0, :, 0:extent], f_ref[1, :, 0:extent])
            green = dot3(split(load(grecv, slot)), cosine)
            green = dot3((ft_ref[0, 0:extent], ft_ref[1, 0:extent]), split(green))
            green = jnp.concatenate([green, green], axis=1)
            green = jnp.concatenate([green, green], axis=0)
            value = dot3(split(load(drecv, slot)), pair(f_ref))
            value = dot3(pair(ft_ref), split(value)) * green
            value = dot3(pair(f_ref), split(value))
            value = dot3(split(value), pair(ft_ref))
            for c in range(ncol):
                for r in range(nrow):
                    start = ((chunk * nsets + r * ncol + c) * each + slot) * groups
                    bsend[pl.ds(start, groups), :] = jnp.concatenate(
                        [
                            value[
                                r * xl + h * groups : r * xl + (h + 1) * groups,
                                c * width : (c + 1) * width,
                            ]
                            for h in range(per)
                        ],
                        axis=1,
                    )
            return inner

        lax.fori_loop(0, each, one_slot, 0)

        def back(step, inner):
            r = lax.rem(row + step, nrow)
            mine = jnp.logical_and(relay_here, r == row)
            for t in range(hc):
                source = rows(bsend, (chunk * nsets + r * ncol + away * hc + t) * size, size)
                start = ((1 + t) * extent + (chunk * team + rank) * each) * groups
                sink = rows(brecv, start, size)

                @pl.when(mine)
                def _():
                    sink[...] = source[...]

                @pl.when(jnp.logical_not(mine))
                def _():
                    remote(
                        source, sink, b_ssem.at[chunk], b_rsem.at[chunk], (r, hc - 1 + half)
                    ).start()

            return inner

        lax.fori_loop(0, nrow, back, 0)
        return carry

    lax.fori_loop(0, chunks, planes, 0)

    def near_back(chunk, carry):
        sink = rows(brecv, (chunk * team + rank) * size, size)

        def one(step, inner):
            target = lax.rem(rank + step, team)
            r, c = lax.div(target, hc), lax.rem(target, hc) + half * hc
            source = rows(bsend, (chunk * nsets + r * ncol + c) * size, size)
            remote(source, sink, n_ssem.at[0], n_rsem.at[0], (r, c)).start()
            return inner

        lax.fori_loop(1, team, one, 0)
        sink[...] = rows(bsend, (chunk * nsets + me) * size, size)[...]
        return carry

    lax.fori_loop(0, chunks, near_back, 0)

    def lines(line, group):
        return split(brecv[pl.ds(line * extent * groups + group, extent, stride=groups), :])

    far_table = (wt_ref[half, 0, 0:mid, :], wt_ref[half, 1, 0:mid, :])

    @pl.when(relay_here)
    def _():
        def settle(chunk, carry):
            wait(brecv, hc * (team - 1) * size, b_rsem.at[chunk])
            return carry

        lax.fori_loop(0, chunks, settle, 0)

        def far_block(b, carry):
            for t in range(hc):
                def far_group(i, inner):
                    g = b * bgroups + i
                    start = pl.multiple_of(g * mid, 8)
                    ret_out[t, pl.ds(start, mid), :] = dot3(far_table, lines(1 + t, g))
                    return inner

                lax.fori_loop(0, bgroups, far_group, 0)
                remote(
                    rows(ret_out.at[t], b * bgroups * mid, bgroups * mid),
                    rows(ret_in, b * bgroups * mid, bgroups * mid),
                    ret_ssem.at[b], ret_rsem.at[b], (row, away * hc + t),
                ).start()
            return carry

        lax.fori_loop(0, blocks, far_block, 0)

    wait(brecv, (team - 1) * chunks * size, n_rsem.at[0])

    def near_group(g, carry):
        start = pl.multiple_of(g * extent, 8)
        total[pl.ds(start, extent), :] = dot3((wt_ref[half, 0], wt_ref[half, 1]), lines(0, g))
        return carry

    lax.fori_loop(0, groups, near_group, 0)

    out_copies = [
        [
            pltpu.make_async_copy(strip(out_ref, b, h), strip(out_hbm, b, h), out_sem.at[b, h])
            for h in range(per)
        ]
        for b in range(blocks)
    ]
    for b in range(blocks):
        view = rows(ret_in, b * bgroups * mid, bgroups * mid)
        pltpu.make_async_copy(view, view, ret_rsem.at[b]).wait()

        def one_group(g, inner):
            high, low = split(ret_in[pl.ds(pl.multiple_of(g * mid, 8), mid), :])
            value = dot(fold_ref[away], high) + dot(fold_ref[away], low)
            value = value + total[pl.ds(pl.multiple_of(g * extent, 8), extent), :]
            value = value.T
            for h in range(per):
                start = pl.multiple_of((h * groups + g) * width, width)
                out_ref[pl.ds(start, width), :] = value[h * width : (h + 1) * width]
            return inner

        lax.fori_loop(b * bgroups, (b + 1) * bgroups, one_group, 0)
        for copy in out_copies[b]:
            copy.start()

    for b in range(blocks):
        wait(raw_out, brows, raw_ssem.at[b])

    wait(brecv, (team - 1) * chunks * size, n_ssem.at[0])

    @pl.when(relay_here)
    def _():
        for b in range(blocks):
            wait(raw_out, hc * bgroups * mid, ret_ssem.at[b])

    def drain(chunk, carry):
        @pl.when(relay_here)
        def _():
            wait(drecv, (nsets - 1 + outer) * size, g_ssem.at[chunk])
            wait(dsend, (1 + hc) * (team - 1) * size, d_ssem.at[chunk])
            wait(bsend, hc * (nrow - 1) * size, b_ssem.at[chunk])

        @pl.when(jnp.logical_not(relay_here))
        def _():
            wait(drecv, (nsets - 1 - nrow) * size, g_ssem.at[chunk])
            wait(dsend, (team - 1) * size, d_ssem.at[chunk])
            wait(bsend, hc * nrow * size, b_ssem.at[chunk])

        return carry

    lax.fori_loop(0, chunks, drain, 0)
    for b in range(blocks):
        for copy in out_copies[b]:
            copy.wait()


def make(mesh):
    nrow, ncol = mesh.shape["row"], mesh.shape["col"]

    def on_device(density, green_octant):
        xl, width, extent = density.shape
        per = 128 // width
        groups = xl // per
        cells = xl * width
        hc = ncol // 2
        team = nrow * hc
        slots = extent // team
        each = min(EACH, slots)
        chunks = slots // each
        blocks = min(BLOCKS, groups)
        mid = extent // 2
        k = np.arange(extent)[:, None]
        n = np.arange(extent)[None, :]
        theta = np.pi / (2 * extent) * (((2 * k + 1) * n) % (4 * extent))
        both = np.concatenate([np.cos(theta), np.sin(theta)], axis=0)
        shifted = np.pi / (4 * extent) * (((2 * k + 1) * (2 * n + 1 - extent)) % (8 * extent))
        waves = np.stack([np.cos(shifted), np.sin(shifted)])
        flip = np.eye(extent)[:, :mid]
        fold = np.stack([flip + flip[::-1], flip - flip[::-1]])
        tables = (
            halves(both.T),
            halves(both),
            halves(waves).transpose(1, 0, 2, 3),
            halves(waves.transpose(0, 2, 1)).transpose(1, 0, 2, 3),
            jnp.asarray(fold.astype(np.float32).astype(BF16)),
        )
        operands = (
            density.reshape(cells, extent),
            green_octant.reshape(cells, extent),
        ) + tables
        sizes = (nrow, ncol, groups, per, width, each, blocks)
        lot = extent * groups
        dma = pltpu.SemaphoreType.DMA
        any_space = pl.BlockSpec(memory_space=pl.ANY)
        out = pl.pallas_call(
            lambda *refs: fused_kernel(sizes, *refs),
            in_specs=[any_space] * len(operands),
            out_specs=any_space,
            out_shape=jax.ShapeDtypeStruct((cells, extent), F32),
            scratch_shapes=[pltpu.VMEM(v.shape, v.dtype) for v in operands]
            + [
                pltpu.VMEM((cells, extent), F32),
                pltpu.VMEM((2, cells, extent), BF16),
                pltpu.VMEM((2, cells, extent), BF16),
                pltpu.VMEM((cells, mid), F32),
                pltpu.VMEM((hc, cells, mid), F32),
                pltpu.VMEM((2, cells, mid), BF16),
                pltpu.VMEM(((1 + hc) * lot, 128), F32),
                pltpu.VMEM((2 * lot, 128), F32),
                pltpu.VMEM((lot, 128), F32),
                pltpu.VMEM((2 * lot, 128), F32),
                pltpu.VMEM((2 * lot, 128), F32),
                pltpu.VMEM(((1 + hc) * lot, 128), F32),
                pltpu.VMEM((hc, groups * mid, 128), F32),
                pltpu.VMEM((groups * mid, 128), F32),
                pltpu.VMEM((groups * extent, 128), F32),
                dma((6,)),
                dma((blocks, per)),
                dma((blocks, per)),
                dma((blocks,)),
                dma((hc, blocks)),
            ]
            + [dma((chunks,))] * 6
            + [dma((blocks,))] * 2
            + [dma((1,))] * 2
            + [dma((chunks,))],
            compiler_params=pltpu.CompilerParams(
                vmem_limit_bytes=VMEM_BYTES, collective_id=0, has_side_effects=True
            ),
            name="fused",
        )(*operands)
        return out.reshape(xl, width, extent)

    return on_device


EACH = 2
BLOCKS = 8
LEAD = 2


def solution(mesh):
    return jax.shard_map(
        make(mesh),
        mesh=mesh,
        in_specs=(P("row", "col", None), P("row", "col", None)),
        out_specs=P("row", "col", None),
        check_vma=False,
    )
```

```python
import jax
import jax.numpy as jnp
import numpy as np
from jax import lax
from jax.experimental import pallas as pl
from jax.experimental.pallas import tpu as pltpu
from jax.sharding import PartitionSpec as P

F32 = jnp.float32
BF16 = jnp.bfloat16
VMEM_BYTES = 62 * 1024 * 1024
MESH = pl.DeviceIdType.MESH


def halves(table):
    table = np.asarray(table, np.float32)
    high = table.astype(BF16)
    low = (table - high.astype(np.float32)).astype(BF16)
    return jnp.asarray(np.stack([high, low]))


def split(value):
    high = value.astype(BF16)
    return high, (value - high.astype(F32)).astype(BF16)


def dot(a, b, dims=((1,), (0,))):
    return lax.dot_general(a, b, (dims, ((), ())), preferred_element_type=F32)


def dot3(left, right, dims=((1,), (0,))):
    return dot(left[0], right[0], dims) + (
        dot(left[0], right[1], dims) + dot(left[1], right[0], dims)
    )


def pair(ref):
    return ref[0], ref[1]


def fused_kernel(sizes, dens_hbm, green_hbm, f_hbm, ft_hbm, w_hbm, wt_hbm, fold_hbm, out_hbm,
                 dens_in, green_in, f_ref, ft_ref, w_ref, wt_ref, fold_ref, out_ref,
                 dens_two, green_two, raw_out, raw_in, far_two, dsend, drecv, gsend, grecv,
                 bsend, brecv, ret_out, ret_in, total, in_sem, dens_sem, out_sem, raw_ssem,
                 raw_rsem, d_ssem, d_rsem, g_ssem, g_rsem, b_ssem, b_rsem, ret_ssem, ret_rsem, n_ssem, n_rsem,
                 o_rsem):
    nrow, ncol, groups, per, width, each, blocks = sizes
    cells, extent = dens_in.shape
    mid = extent // 2
    xl = groups * per
    hc = ncol // 2
    nsets = nrow * ncol
    team = nrow * hc
    chunks = extent // (team * each)
    row, col = lax.axis_index("row"), lax.axis_index("col")
    me = row * ncol + col
    half = lax.div(col, hc)
    away = 1 - half
    spot = col - half * hc
    rank = row * hc + spot
    relay_spot = (hc - 1) * away
    relay_here = spot == relay_spot
    outer = nrow * (hc - 1)
    size = each * groups
    bgroups = groups // blocks
    brows = bgroups * 128

    def place(index):
        return lax.div(index, ncol), lax.rem(index, ncol)

    def greet(step, carry):
        pl.semaphore_signal(
            barrier, inc=1, device_id=place(lax.rem(me + step, nsets)), device_id_type=MESH
        )
        return carry

    barrier = pltpu.get_barrier_semaphore()
    lax.fori_loop(1, nsets, greet, 0)

    def strip(ref, b, h):
        start = (h * groups + b * bgroups) * width
        return ref.at[pl.ds(start, bgroups * width), :]

    dens_copies = [
        [
            pltpu.make_async_copy(strip(dens_hbm, b, h), strip(dens_in, b, h), dens_sem.at[b, h])
            for h in range(per)
        ]
        for b in range(blocks)
    ]
    copies = [
        pltpu.make_async_copy(source, target, in_sem.at[i])
        for i, (source, target) in enumerate(
            (
                (fold_hbm, fold_ref),
                (w_hbm, w_ref),
                (green_hbm, green_in),
                (ft_hbm, ft_ref),
                (f_hbm, f_ref),
                (wt_hbm, wt_ref),
            )
        )
    ]
    copies[0].start()
    for b in range(blocks):
        for copy in dens_copies[b]:
            copy.start()
    for copy in copies[1:]:
        copy.start()

    def remote(source, target, send_sem, recv_sem, device):
        return pltpu.make_async_remote_copy(
            src_ref=source,
            dst_ref=target,
            send_sem=send_sem,
            recv_sem=recv_sem,
            device_id=device,
            device_id_type=MESH,
        )

    def rows(ref, start, length):
        return ref.at[pl.ds(pl.multiple_of(start, 8), length), :]

    def wait(ref, length, sem):
        view = ref.at[pl.ds(0, length), :]
        pltpu.make_async_copy(view, view, sem).wait()

    def pick(ref, g):
        return jnp.concatenate(
            [
                ref[pl.ds(pl.multiple_of((h * groups + g) * width, width), width), :]
                for h in range(per)
            ],
            axis=0,
        )

    def fold(g, carry):
        start = pl.multiple_of(g * 128, 128)
        high, low = split(pick(dens_in, g))
        dens_two[0, pl.ds(start, 128), :] = high
        dens_two[1, pl.ds(start, 128), :] = low
        raw_out[pl.ds(start, 128), :] = dot(high, fold_ref[away]) + dot(low, fold_ref[away])
        return carry

    copies[0].wait()
    for b in range(blocks):
        for copy in dens_copies[b]:
            copy.wait()
        lax.fori_loop(b * bgroups, (b + 1) * bgroups, fold, 0)
        if b == 0:
            pl.semaphore_wait(barrier, nsets - 1)
        remote(
            rows(raw_out, b * brows, brows), rows(raw_in.at[spot], b * brows, brows),
            raw_ssem.at[b], raw_rsem.at[spot, b], (row, hc - 1 + away),
        ).start()

    def transform(two, table, send, line):
        def tile(t, carry):
            start = pl.multiple_of(t * 256, 256)
            right = (two[0, pl.ds(start, 256), :], two[1, pl.ds(start, 256), :])
            result = dot3(table, right, ((1,), (1,)))
            for i in range(2):
                send[pl.ds(line * extent * groups + t * 2 + i, extent, stride=groups), :] = (
                    result[:, i * 128 : (i + 1) * 128]
                )
            return carry

        lax.fori_loop(0, cells // 256, tile, 0)

    copies[1].wait()
    transform(dens_two, (w_ref[half, 0], w_ref[half, 1]), dsend, 0)

    def scatter_dens(lines_sets):
        def one_chunk(chunk, outer):
            def one(step, carry):
                target = lax.rem(rank + step, team)
                device = (lax.div(target, hc), lax.rem(target, hc) + half * hc)
                for line, sets in lines_sets:
                    remote(
                        rows(
                            dsend, (line * extent + (chunk * team + target) * each) * groups, size
                        ),
                        rows(drecv, (chunk * nsets + sets) * size, size),
                        d_ssem.at[chunk], d_rsem.at[chunk], device,
                    ).start()
                return carry

            lax.fori_loop(1, team, one, 0)
            for line, sets in lines_sets:
                rows(drecv, (chunk * nsets + sets) * size, size)[...] = rows(
                    dsend, (line * extent + (chunk * team + rank) * each) * groups, size
                )[...]
            return outer

        lax.fori_loop(0, chunks, one_chunk, 0)

    scatter_dens([(0, me)])

    def weigh(g, carry):
        cell = lax.broadcasted_iota(jnp.int32, (128, extent), 0)
        z = lax.broadcasted_iota(jnp.int32, (128, extent), 1)
        lane_h = lax.div(cell, width)
        y = cell - lane_h * width + col * width
        x = lane_h * groups + g + row * xl
        weight = jnp.where(x == 0, 1.0, 2.0) * jnp.where(y == 0, 1.0, 2.0)
        weight = weight * jnp.where(z == 0, 1.0, 2.0) * (1.0 / (extent * extent * extent))
        start = pl.multiple_of(g * 128, 128)
        high, low = split(pick(green_in, g) * weight)
        green_two[0, pl.ds(start, 128), :] = high
        green_two[1, pl.ds(start, 128), :] = low
        return carry

    copies[2].wait()
    copies[3].wait()
    lax.fori_loop(0, groups, weigh, 0)
    transform(green_two, (ft_ref[0, 0:extent], ft_ref[1, 0:extent]), gsend, 0)

    def green_to(chunk, r, s, side, sem):
        remote(
            rows(gsend, (chunk * team + r * hc + s) * size, size),
            rows(grecv, (chunk * nsets + me) * size, size),
            g_ssem.at[chunk], sem.at[chunk], (r, s + side * hc),
        ).start()

    def green_inside(chunk, carry):
        def one(step, inner):
            target = lax.rem(rank + step, team)
            r, s = lax.div(target, hc), lax.rem(target, hc)
            via = jnp.logical_and(jnp.logical_not(relay_here), s == relay_spot)

            @pl.when(via)
            def _():
                green_to(chunk, r, s, half, o_rsem)

            @pl.when(jnp.logical_not(via))
            def _():
                green_to(chunk, r, s, half, g_rsem)

            return inner

        lax.fori_loop(1, team, one, 0)
        rows(grecv, (chunk * nsets + me) * size, size)[...] = rows(
            gsend, (chunk * team + rank) * size, size
        )[...]
        return carry

    def green_away(chunk, carry):
        def one(step, inner):
            target = lax.rem(rank + step, team)
            r, s = lax.div(target, hc), lax.rem(target, hc)

            @pl.when(jnp.logical_or(relay_here, s != relay_spot))
            def _():
                green_to(chunk, r, s, away, g_rsem)

            return inner

        lax.fori_loop(0, team, one, 0)
        return carry

    def hand_on(chunk):
        wait(grecv, outer * size, o_rsem.at[chunk])
        for i in range(hc - 1):
            s = i + lax.convert_element_type(relay_spot <= i, jnp.int32)

            def one(r, inner):
                block = rows(grecv, (chunk * nsets + r * ncol + half * hc + s) * size, size)
                remote(
                    block, block, g_ssem.at[chunk], g_rsem.at[chunk],
                    (row, away * hc + relay_spot),
                ).start()
                return inner

            lax.fori_loop(0, nrow, one, 0)

    def pace(chunk):
        @pl.when(jnp.logical_and(relay_here, chunk < chunks))
        def _():
            hand_on(chunk)

        @pl.when(jnp.logical_and(relay_here, chunk + LEAD < chunks))
        def _():
            green_away(chunk + LEAD, 0)

    lead = jnp.where(relay_here, min(LEAD, chunks), chunks)

    def green_first(chunk, carry):
        green_inside(chunk, 0)

        @pl.when(chunk < lead)
        def _():
            green_away(chunk, 0)

        return carry

    lax.fori_loop(0, chunks, green_first, 0)
    copies[4].wait()
    copies[5].wait()

    @pl.when(relay_here)
    def _():
        for t in range(hc):
            for b in range(blocks):
                view = rows(raw_in.at[t], b * brows, brows)
                pltpu.make_async_copy(view, view, raw_rsem.at[t, b]).wait()
                high, low = split(view[...])
                far_two[0, pl.ds(b * brows, brows), :] = high
                far_two[1, pl.ds(b * brows, brows), :] = low
            w_far = (w_ref[half, 0, :, 0:mid], w_ref[half, 1, :, 0:mid])
            transform(far_two, w_far, dsend, 1 + t)
        scatter_dens([(1 + t, row * ncol + away * hc + t) for t in range(hc)])

    pace(0)

    def planes(chunk, carry):
        pace(chunk + 1)

        @pl.when(relay_here)
        def _():
            wait(drecv, (nsets - 1 - hc) * size, d_rsem.at[chunk])
            wait(grecv, (nsets - 1 - outer) * size, g_rsem.at[chunk])

        @pl.when(jnp.logical_not(relay_here))
        def _():
            wait(drecv, (nsets - 1) * size, d_rsem.at[chunk])
            wait(grecv, (nsets - 1) * size, g_rsem.at[chunk])

        def load(ref, slot):
            def piece(r, c):
                start = ((chunk * nsets + r * ncol + c) * each + slot) * groups
                return ref[pl.ds(start, groups), :]

            columns = [
                jnp.concatenate([piece(r, c) for r in range(nrow)], axis=0) for c in range(ncol)
            ]
            layers = [
                jnp.concatenate([v[:, h * width : (h + 1) * width] for v in columns], axis=1)
                for h in range(per)
            ]
            return jnp.concatenate(
                [v[r * groups : (r + 1) * groups] for r in range(nrow) for v in layers], axis=0
            )

        def one_slot(slot, inner):
            cosine = (f_ref[0, :, 0:extent], f_ref[1, :, 0:extent])
            green = dot3(split(load(grecv, slot)), cosine)
            green = dot3((ft_ref[0, 0:extent], ft_ref[1, 0:extent]), split(green))
            green = jnp.concatenate([green, green], axis=1)
            green = jnp.concatenate([green, green], axis=0)
            value = dot3(split(load(drecv, slot)), pair(f_ref))
            value = dot3(pair(ft_ref), split(value)) * green
            value = dot3(pair(f_ref), split(value))
            value = dot3(split(value), pair(ft_ref))
            for c in range(ncol):
                for r in range(nrow):
                    start = ((chunk * nsets + r * ncol + c) * each + slot) * groups
                    bsend[pl.ds(start, groups), :] = jnp.concatenate(
                        [
                            value[
                                r * xl + h * groups : r * xl + (h + 1) * groups,
                                c * width : (c + 1) * width,
                            ]
                            for h in range(per)
                        ],
                        axis=1,
                    )
            return inner

        lax.fori_loop(0, each, one_slot, 0)

        def back(step, inner):
            r = lax.rem(row + step, nrow)
            mine = jnp.logical_and(relay_here, r == row)
            for t in range(hc):
                source = rows(bsend, (chunk * nsets + r * ncol + away * hc + t) * size, size)
                start = ((1 + t) * extent + (chunk * team + rank) * each) * groups
                sink = rows(brecv, start, size)

                @pl.when(mine)
                def _():
                    sink[...] = source[...]

                @pl.when(jnp.logical_not(mine))
                def _():
                    remote(
                        source, sink, b_ssem.at[chunk], b_rsem.at[chunk], (r, hc - 1 + half)
                    ).start()

            return inner

        lax.fori_loop(0, nrow, back, 0)
        return carry

    lax.fori_loop(0, chunks, planes, 0)

    def near_back(chunk, carry):
        sink = rows(brecv, (chunk * team + rank) * size, size)

        def one(step, inner):
            target = lax.rem(rank + step, team)
            r, c = lax.div(target, hc), lax.rem(target, hc) + half * hc
            source = rows(bsend, (chunk * nsets + r * ncol + c) * size, size)
            remote(source, sink, n_ssem.at[0], n_rsem.at[0], (r, c)).start()
            return inner

        lax.fori_loop(1, team, one, 0)
        sink[...] = rows(bsend, (chunk * nsets + me) * size, size)[...]
        return carry

    lax.fori_loop(0, chunks, near_back, 0)

    def lines(line, group):
        return split(brecv[pl.ds(line * extent * groups + group, extent, stride=groups), :])

    far_table = (wt_ref[half, 0, 0:mid, :], wt_ref[half, 1, 0:mid, :])

    @pl.when(relay_here)
    def _():
        def settle(chunk, carry):
            wait(brecv, hc * (team - 1) * size, b_rsem.at[chunk])
            return carry

        lax.fori_loop(0, chunks, settle, 0)

        def far_block(b, carry):
            for t in range(hc):
                def far_group(i, inner):
                    g = b * bgroups + i
                    start = pl.multiple_of(g * mid, 8)
                    ret_out[t, pl.ds(start, mid), :] = dot3(far_table, lines(1 + t, g))
                    return inner

                lax.fori_loop(0, bgroups, far_group, 0)
                remote(
                    rows(ret_out.at[t], b * bgroups * mid, bgroups * mid),
                    rows(ret_in, b * bgroups * mid, bgroups * mid),
                    ret_ssem.at[b], ret_rsem.at[b], (row, away * hc + t),
                ).start()
            return carry

        lax.fori_loop(0, blocks, far_block, 0)

    wait(brecv, (team - 1) * chunks * size, n_rsem.at[0])

    def near_group(g, carry):
        start = pl.multiple_of(g * extent, 8)
        total[pl.ds(start, extent), :] = dot3((wt_ref[half, 0], wt_ref[half, 1]), lines(0, g))
        return carry

    lax.fori_loop(0, groups, near_group, 0)

    out_copies = [
        [
            pltpu.make_async_copy(strip(out_ref, b, h), strip(out_hbm, b, h), out_sem.at[b, h])
            for h in range(per)
        ]
        for b in range(blocks)
    ]
    for b in range(blocks):
        view = rows(ret_in, b * bgroups * mid, bgroups * mid)
        pltpu.make_async_copy(view, view, ret_rsem.at[b]).wait()

        def one_group(g, inner):
            high, low = split(ret_in[pl.ds(pl.multiple_of(g * mid, 8), mid), :])
            value = dot(fold_ref[away], high) + dot(fold_ref[away], low)
            value = value + total[pl.ds(pl.multiple_of(g * extent, 8), extent), :]
            value = value.T
            for h in range(per):
                start = pl.multiple_of((h * groups + g) * width, width)
                out_ref[pl.ds(start, width), :] = value[h * width : (h + 1) * width]
            return inner

        lax.fori_loop(b * bgroups, (b + 1) * bgroups, one_group, 0)
        for copy in out_copies[b]:
            copy.start()

    for b in range(blocks):
        wait(raw_out, brows, raw_ssem.at[b])

    wait(brecv, (team - 1) * chunks * size, n_ssem.at[0])

    @pl.when(relay_here)
    def _():
        for b in range(blocks):
            wait(raw_out, hc * bgroups * mid, ret_ssem.at[b])

    def drain(chunk, carry):
        @pl.when(relay_here)
        def _():
            wait(drecv, (nsets - 1 + outer) * size, g_ssem.at[chunk])
            wait(dsend, (1 + hc) * (team - 1) * size, d_ssem.at[chunk])
            wait(bsend, hc * (nrow - 1) * size, b_ssem.at[chunk])

        @pl.when(jnp.logical_not(relay_here))
        def _():
            wait(drecv, (nsets - 1 - nrow) * size, g_ssem.at[chunk])
            wait(dsend, (team - 1) * size, d_ssem.at[chunk])
            wait(bsend, hc * nrow * size, b_ssem.at[chunk])

        return carry

    lax.fori_loop(0, chunks, drain, 0)
    for b in range(blocks):
        for copy in out_copies[b]:
            copy.wait()


def make(mesh):
    nrow, ncol = mesh.shape["row"], mesh.shape["col"]

    def on_device(density, green_octant):
        xl, width, extent = density.shape
        per = 128 // width
        groups = xl // per
        cells = xl * width
        hc = ncol // 2
        team = nrow * hc
        slots = extent // team
        each = min(max(EACH, 8 // groups), slots)
        chunks = slots // each
        blocks = min(BLOCKS, groups)
        mid = extent // 2
        k = np.arange(extent)[:, None]
        n = np.arange(extent)[None, :]
        theta = np.pi / (2 * extent) * (((2 * k + 1) * n) % (4 * extent))
        both = np.concatenate([np.cos(theta), np.sin(theta)], axis=0)
        shifted = np.pi / (4 * extent) * (((2 * k + 1) * (2 * n + 1 - extent)) % (8 * extent))
        waves = np.stack([np.cos(shifted), np.sin(shifted)])
        flip = np.eye(extent)[:, :mid]
        fold = np.stack([flip + flip[::-1], flip - flip[::-1]])
        tables = (
            halves(both.T),
            halves(both),
            halves(waves).transpose(1, 0, 2, 3),
            halves(waves.transpose(0, 2, 1)).transpose(1, 0, 2, 3),
            jnp.asarray(fold.astype(np.float32).astype(BF16)),
        )
        operands = (
            density.reshape(cells, extent),
            green_octant.reshape(cells, extent),
        ) + tables
        sizes = (nrow, ncol, groups, per, width, each, blocks)
        lot = extent * groups
        dma = pltpu.SemaphoreType.DMA
        any_space = pl.BlockSpec(memory_space=pl.ANY)
        out = pl.pallas_call(
            lambda *refs: fused_kernel(sizes, *refs),
            in_specs=[any_space] * len(operands),
            out_specs=any_space,
            out_shape=jax.ShapeDtypeStruct((cells, extent), F32),
            scratch_shapes=[pltpu.VMEM(v.shape, v.dtype) for v in operands]
            + [
                pltpu.VMEM((cells, extent), F32),
                pltpu.VMEM((2, cells, extent), BF16),
                pltpu.VMEM((2, cells, extent), BF16),
                pltpu.VMEM((cells, mid), F32),
                pltpu.VMEM((hc, cells, mid), F32),
                pltpu.VMEM((2, cells, mid), BF16),
                pltpu.VMEM(((1 + hc) * lot, 128), F32),
                pltpu.VMEM((2 * lot, 128), F32),
                pltpu.VMEM((lot, 128), F32),
                pltpu.VMEM((2 * lot, 128), F32),
                pltpu.VMEM((2 * lot, 128), F32),
                pltpu.VMEM(((1 + hc) * lot, 128), F32),
                pltpu.VMEM((hc, groups * mid, 128), F32),
                pltpu.VMEM((groups * mid, 128), F32),
                pltpu.VMEM((groups * extent, 128), F32),
                dma((6,)),
                dma((blocks, per)),
                dma((blocks, per)),
                dma((blocks,)),
                dma((hc, blocks)),
            ]
            + [dma((chunks,))] * 6
            + [dma((blocks,))] * 2
            + [dma((1,))] * 2
            + [dma((chunks,))],
            compiler_params=pltpu.CompilerParams(
                vmem_limit_bytes=VMEM_BYTES, collective_id=0, has_side_effects=True
            ),
            name="fused",
        )(*operands)
        return out.reshape(xl, width, extent)

    return on_device


EACH = 1
BLOCKS = 8
LEAD = 4


def solution(mesh):
    return jax.shard_map(
        make(mesh),
        mesh=mesh,
        in_specs=(P("row", "col", None), P("row", "col", None)),
        out_specs=P("row", "col", None),
        check_vma=False,
    )
```

```python
import jax
import jax.numpy as jnp
import numpy as np
from jax import lax
from jax.experimental import pallas as pl
from jax.experimental.pallas import tpu as pltpu
from jax.sharding import PartitionSpec as P

F32 = jnp.float32
BF16 = jnp.bfloat16
VMEM_BYTES = 62 * 1024 * 1024
MESH = pl.DeviceIdType.MESH


def halves(table):
    table = np.asarray(table, np.float32)
    high = table.astype(BF16)
    low = (table - high.astype(np.float32)).astype(BF16)
    return jnp.asarray(np.stack([high, low]))


def split(value):
    high = value.astype(BF16)
    return high, (value - high.astype(F32)).astype(BF16)


def dot(a, b, dims=((1,), (0,))):
    return lax.dot_general(a, b, (dims, ((), ())), preferred_element_type=F32)


def dot3(left, right, dims=((1,), (0,))):
    return dot(left[0], right[0], dims) + (
        dot(left[0], right[1], dims) + dot(left[1], right[0], dims)
    )


def pair(ref):
    return ref[0], ref[1]


def fused_kernel(sizes, dens_hbm, green_hbm, f_hbm, ft_hbm, w_hbm, wt_hbm, fold_hbm, out_hbm,
                 dens_in, green_in, f_ref, ft_ref, w_ref, wt_ref, fold_ref, out_ref,
                 dens_two, green_two, raw_out, raw_in, dsend, drecv, gsend, grecv,
                 bsend, brecv, ret_out, ret_in, total, in_sem, dens_sem, out_sem, raw_ssem,
                 raw_rsem, d_ssem, d_rsem, g_ssem, g_rsem, b_ssem, b_rsem, ret_ssem, ret_rsem, n_ssem, n_rsem,
                 o_rsem):
    nrow, ncol, groups, per, width, each, blocks = sizes
    cells, extent = dens_in.shape
    mid = extent // 2
    xl = groups * per
    hc = ncol // 2
    nsets = nrow * ncol
    team = nrow * hc
    chunks = extent // (team * each)
    row, col = lax.axis_index("row"), lax.axis_index("col")
    me = row * ncol + col
    half = lax.div(col, hc)
    away = 1 - half
    spot = col - half * hc
    rank = row * hc + spot
    relay_spot = (hc - 1) * away
    relay_here = spot == relay_spot
    outer = nrow * (hc - 1)
    size = each * groups
    bgroups = groups // blocks
    brows = bgroups * 128

    def place(index):
        return lax.div(index, ncol), lax.rem(index, ncol)

    def greet(step, carry):
        pl.semaphore_signal(
            barrier, inc=1, device_id=place(lax.rem(me + step, nsets)), device_id_type=MESH
        )
        return carry

    barrier = pltpu.get_barrier_semaphore()
    lax.fori_loop(1, nsets, greet, 0)

    def strip(ref, b, h):
        start = (h * groups + b * bgroups) * width
        return ref.at[pl.ds(start, bgroups * width), :]

    dens_copies = [
        [
            pltpu.make_async_copy(strip(dens_hbm, b, h), strip(dens_in, b, h), dens_sem.at[b, h])
            for h in range(per)
        ]
        for b in range(blocks)
    ]
    copies = [
        pltpu.make_async_copy(source, target, in_sem.at[i])
        for i, (source, target) in enumerate(
            (
                (fold_hbm, fold_ref),
                (w_hbm, w_ref),
                (green_hbm, green_in),
                (ft_hbm, ft_ref),
                (f_hbm, f_ref),
                (wt_hbm, wt_ref),
            )
        )
    ]
    copies[0].start()
    for b in range(blocks):
        for copy in dens_copies[b]:
            copy.start()
    for copy in copies[1:]:
        copy.start()

    def remote(source, target, send_sem, recv_sem, device):
        return pltpu.make_async_remote_copy(
            src_ref=source,
            dst_ref=target,
            send_sem=send_sem,
            recv_sem=recv_sem,
            device_id=device,
            device_id_type=MESH,
        )

    def rows(ref, start, length):
        return ref.at[pl.ds(pl.multiple_of(start, 8), length), :]

    def wait(ref, length, sem):
        view = ref.at[pl.ds(0, length), :]
        pltpu.make_async_copy(view, view, sem).wait()

    def pick(ref, g):
        return jnp.concatenate(
            [
                ref[pl.ds(pl.multiple_of((h * groups + g) * width, width), width), :]
                for h in range(per)
            ],
            axis=0,
        )

    def fold(g, carry):
        start = pl.multiple_of(g * 128, 128)
        high, low = split(pick(dens_in, g))
        dens_two[0, pl.ds(start, 128), :] = high
        dens_two[1, pl.ds(start, 128), :] = low
        raw_out[pl.ds(start, 128), :] = dot(high, fold_ref[away]) + dot(low, fold_ref[away])
        return carry

    copies[0].wait()
    for b in range(blocks):
        for copy in dens_copies[b]:
            copy.wait()
        lax.fori_loop(b * bgroups, (b + 1) * bgroups, fold, 0)
        if b == 0:
            pl.semaphore_wait(barrier, nsets - 1)
        remote(
            rows(raw_out, b * brows, brows), rows(raw_in.at[spot], b * brows, brows),
            raw_ssem.at[b], raw_rsem.at[spot, b], (row, hc - 1 + away),
        ).start()

    def transform(two, table, send, first):
        count = table[0].shape[0]

        def tile(t, carry):
            start = pl.multiple_of(t * 256, 256)
            right = (two[0, pl.ds(start, 256), :], two[1, pl.ds(start, 256), :])
            result = dot3(table, right, ((1,), (1,)))
            for i in range(2):
                send[pl.ds(first * groups + t * 2 + i, count, stride=groups), :] = (
                    result[:, i * 128 : (i + 1) * 128]
                )
            return carry

        lax.fori_loop(0, cells // 256, tile, 0)

    copies[1].wait()

    def scatter_dens(lines_sets, begin, end):
        def one_chunk(chunk, outer):
            def one(step, carry):
                target = lax.rem(rank + step, team)
                device = (lax.div(target, hc), lax.rem(target, hc) + half * hc)
                for line, sets in lines_sets:
                    remote(
                        rows(
                            dsend, (line * extent + (chunk * team + target) * each) * groups, size
                        ),
                        rows(drecv, (chunk * nsets + sets) * size, size),
                        d_ssem.at[chunk], d_rsem.at[chunk], device,
                    ).start()
                return carry

            lax.fori_loop(1, team, one, 0)
            for line, sets in lines_sets:
                rows(drecv, (chunk * nsets + sets) * size, size)[...] = rows(
                    dsend, (line * extent + (chunk * team + rank) * each) * groups, size
                )[...]
            return outer

        lax.fori_loop(begin, end, one_chunk, 0)

    stages = 2 if chunks % 2 == 0 else 1
    stage = extent // stages
    for i in range(stages):
        w_part = tuple(w_ref[half, j, i * stage : (i + 1) * stage, :] for j in range(2))
        transform(dens_two, w_part, dsend, i * stage)
        scatter_dens([(0, me)], i * chunks // stages, (i + 1) * chunks // stages)

    def weigh(g, carry):
        cell = lax.broadcasted_iota(jnp.int32, (128, extent), 0)
        z = lax.broadcasted_iota(jnp.int32, (128, extent), 1)
        lane_h = lax.div(cell, width)
        y = cell - lane_h * width + col * width
        x = lane_h * groups + g + row * xl
        weight = jnp.where(x == 0, 1.0, 2.0) * jnp.where(y == 0, 1.0, 2.0)
        weight = weight * jnp.where(z == 0, 1.0, 2.0) * (1.0 / (extent * extent * extent))
        start = pl.multiple_of(g * 128, 128)
        high, low = split(pick(green_in, g) * weight)
        green_two[0, pl.ds(start, 128), :] = high
        green_two[1, pl.ds(start, 128), :] = low
        return carry

    copies[2].wait()
    copies[3].wait()
    lax.fori_loop(0, groups, weigh, 0)
    transform(green_two, (ft_ref[0, 0:extent], ft_ref[1, 0:extent]), gsend, 0)

    def green_to(chunk, r, s, side, sem):
        remote(
            rows(gsend, (chunk * team + r * hc + s) * size, size),
            rows(grecv, (chunk * nsets + me) * size, size),
            g_ssem.at[chunk], sem.at[chunk], (r, s + side * hc),
        ).start()

    def green_inside(chunk, carry):
        def one(step, inner):
            target = lax.rem(rank + step, team)
            r, s = lax.div(target, hc), lax.rem(target, hc)
            via = jnp.logical_and(jnp.logical_not(relay_here), s == relay_spot)

            @pl.when(via)
            def _():
                green_to(chunk, r, s, half, o_rsem)

            @pl.when(jnp.logical_not(via))
            def _():
                green_to(chunk, r, s, half, g_rsem)

            return inner

        lax.fori_loop(1, team, one, 0)
        rows(grecv, (chunk * nsets + me) * size, size)[...] = rows(
            gsend, (chunk * team + rank) * size, size
        )[...]
        return carry

    def green_away(chunk, carry):
        def one(step, inner):
            target = lax.rem(rank + step, team)
            r, s = lax.div(target, hc), lax.rem(target, hc)

            @pl.when(jnp.logical_or(relay_here, s != relay_spot))
            def _():
                green_to(chunk, r, s, away, g_rsem)

            return inner

        lax.fori_loop(0, team, one, 0)
        return carry

    def hand_on(chunk):
        wait(grecv, outer * size, o_rsem.at[chunk])
        for i in range(hc - 1):
            s = i + lax.convert_element_type(relay_spot <= i, jnp.int32)

            def one(r, inner):
                block = rows(grecv, (chunk * nsets + r * ncol + half * hc + s) * size, size)
                remote(
                    block, block, g_ssem.at[chunk], g_rsem.at[chunk],
                    (row, away * hc + relay_spot),
                ).start()
                return inner

            lax.fori_loop(0, nrow, one, 0)

    def pace(chunk):
        @pl.when(jnp.logical_and(relay_here, chunk < chunks))
        def _():
            hand_on(chunk)

        @pl.when(jnp.logical_and(relay_here, chunk + LEAD < chunks))
        def _():
            green_away(chunk + LEAD, 0)

    lead = jnp.where(relay_here, min(LEAD, chunks), chunks)

    def green_first(chunk, carry):
        green_inside(chunk, 0)

        @pl.when(chunk < lead)
        def _():
            green_away(chunk, 0)

        return carry

    lax.fori_loop(0, chunks, green_first, 0)
    copies[4].wait()
    copies[5].wait()

    @pl.when(relay_here)
    def _():
        w_far = (w_ref[half, 0, :, 0:mid], w_ref[half, 1, :, 0:mid])

        def far_lines(b, carry):
            for t in range(hc):
                view = rows(raw_in.at[t], b * brows, brows)
                pltpu.make_async_copy(view, view, raw_rsem.at[t, b]).wait()
                result = dot3(w_far, split(view[...]), ((1,), (1,)))
                for i in range(bgroups):
                    start = (1 + t) * extent * groups + b * bgroups + i
                    dsend[pl.ds(start, extent, stride=groups), :] = (
                        result[:, i * 128 : (i + 1) * 128]
                    )
            return carry

        lax.fori_loop(0, blocks, far_lines, 0)
        scatter_dens([(1 + t, row * ncol + away * hc + t) for t in range(hc)], 0, chunks)

    pace(0)

    def planes(chunk, carry):
        pace(chunk + 1)

        @pl.when(relay_here)
        def _():
            wait(drecv, (nsets - 1 - hc) * size, d_rsem.at[chunk])
            wait(grecv, (nsets - 1 - outer) * size, g_rsem.at[chunk])

        @pl.when(jnp.logical_not(relay_here))
        def _():
            wait(drecv, (nsets - 1) * size, d_rsem.at[chunk])
            wait(grecv, (nsets - 1) * size, g_rsem.at[chunk])

        def load(ref, slot):
            def piece(r, c):
                start = ((chunk * nsets + r * ncol + c) * each + slot) * groups
                return ref[pl.ds(start, groups), :]

            columns = [
                jnp.concatenate([piece(r, c) for r in range(nrow)], axis=0) for c in range(ncol)
            ]
            layers = [
                jnp.concatenate([v[:, h * width : (h + 1) * width] for v in columns], axis=1)
                for h in range(per)
            ]
            return jnp.concatenate(
                [v[r * groups : (r + 1) * groups] for r in range(nrow) for v in layers], axis=0
            )

        def one_slot(slot, inner):
            cosine = (f_ref[0, :, 0:extent], f_ref[1, :, 0:extent])
            green = dot3(split(load(grecv, slot)), cosine)
            green = dot3((ft_ref[0, 0:extent], ft_ref[1, 0:extent]), split(green))
            green = jnp.concatenate([green, green], axis=1)
            green = jnp.concatenate([green, green], axis=0)
            value = dot3(split(load(drecv, slot)), pair(f_ref))
            value = dot3(pair(ft_ref), split(value)) * green
            value = dot3(pair(f_ref), split(value))
            value = dot3(split(value), pair(ft_ref))
            for c in range(ncol):
                for r in range(nrow):
                    start = ((chunk * nsets + r * ncol + c) * each + slot) * groups
                    bsend[pl.ds(start, groups), :] = jnp.concatenate(
                        [
                            value[
                                r * xl + h * groups : r * xl + (h + 1) * groups,
                                c * width : (c + 1) * width,
                            ]
                            for h in range(per)
                        ],
                        axis=1,
                    )
            return inner

        lax.fori_loop(0, each, one_slot, 0)

        def back(step, inner):
            r = lax.rem(row + step, nrow)
            mine = jnp.logical_and(relay_here, r == row)
            for t in range(hc):
                source = rows(bsend, (chunk * nsets + r * ncol + away * hc + t) * size, size)
                start = ((1 + t) * extent + (chunk * team + rank) * each) * groups
                sink = rows(brecv, start, size)

                @pl.when(mine)
                def _():
                    sink[...] = source[...]

                @pl.when(jnp.logical_not(mine))
                def _():
                    remote(
                        source, sink, b_ssem.at[chunk], b_rsem.at[chunk], (r, hc - 1 + half)
                    ).start()

            return inner

        lax.fori_loop(0, nrow, back, 0)
        return carry

    lax.fori_loop(0, chunks, planes, 0)

    def near_back(chunk, carry):
        sink = rows(brecv, (chunk * team + rank) * size, size)

        def one(step, inner):
            target = lax.rem(rank + step, team)
            r, c = lax.div(target, hc), lax.rem(target, hc) + half * hc
            source = rows(bsend, (chunk * nsets + r * ncol + c) * size, size)
            remote(source, sink, n_ssem.at[0], n_rsem.at[0], (r, c)).start()
            return inner

        lax.fori_loop(1, team, one, 0)
        sink[...] = rows(bsend, (chunk * nsets + me) * size, size)[...]
        return carry

    lax.fori_loop(0, chunks, near_back, 0)

    def lines(line, group):
        return split(brecv[pl.ds(line * extent * groups + group, extent, stride=groups), :])

    far_table = (wt_ref[half, 0, 0:mid, :], wt_ref[half, 1, 0:mid, :])

    @pl.when(relay_here)
    def _():
        def settle(chunk, carry):
            wait(brecv, hc * (team - 1) * size, b_rsem.at[chunk])
            return carry

        lax.fori_loop(0, chunks, settle, 0)

        def far_block(b, carry):
            for t in range(hc):
                def far_group(i, inner):
                    g = b * bgroups + i
                    start = pl.multiple_of(g * mid, 8)
                    ret_out[t, pl.ds(start, mid), :] = dot3(far_table, lines(1 + t, g))
                    return inner

                lax.fori_loop(0, bgroups, far_group, 0)
                remote(
                    rows(ret_out.at[t], b * bgroups * mid, bgroups * mid),
                    rows(ret_in, b * bgroups * mid, bgroups * mid),
                    ret_ssem.at[b], ret_rsem.at[b], (row, away * hc + t),
                ).start()
            return carry

        lax.fori_loop(0, blocks, far_block, 0)

    wait(brecv, (team - 1) * chunks * size, n_rsem.at[0])

    def near_group(g, carry):
        start = pl.multiple_of(g * extent, 8)
        total[pl.ds(start, extent), :] = dot3((wt_ref[half, 0], wt_ref[half, 1]), lines(0, g))
        return carry

    lax.fori_loop(0, groups, near_group, 0)

    for b in range(blocks):
        wait(raw_out, brows, raw_ssem.at[b])

    wait(brecv, (team - 1) * chunks * size, n_ssem.at[0])

    def drain(chunk, carry):
        @pl.when(relay_here)
        def _():
            wait(drecv, (nsets - 1 + outer) * size, g_ssem.at[chunk])
            wait(dsend, (1 + hc) * (team - 1) * size, d_ssem.at[chunk])
            wait(bsend, hc * (nrow - 1) * size, b_ssem.at[chunk])

        @pl.when(jnp.logical_not(relay_here))
        def _():
            wait(drecv, (nsets - 1 - nrow) * size, g_ssem.at[chunk])
            wait(dsend, (team - 1) * size, d_ssem.at[chunk])
            wait(bsend, hc * nrow * size, b_ssem.at[chunk])

        return carry

    lax.fori_loop(0, chunks, drain, 0)

    out_copies = [
        [
            pltpu.make_async_copy(strip(out_ref, b, h), strip(out_hbm, b, h), out_sem.at[b, h])
            for h in range(per)
        ]
        for b in range(blocks)
    ]
    for b in range(blocks):
        view = rows(ret_in, b * bgroups * mid, bgroups * mid)
        pltpu.make_async_copy(view, view, ret_rsem.at[b]).wait()

        def one_group(g, inner):
            high, low = split(ret_in[pl.ds(pl.multiple_of(g * mid, 8), mid), :])
            value = dot(fold_ref[away], high) + dot(fold_ref[away], low)
            value = value + total[pl.ds(pl.multiple_of(g * extent, 8), extent), :]
            value = value.T
            for h in range(per):
                start = pl.multiple_of((h * groups + g) * width, width)
                out_ref[pl.ds(start, width), :] = value[h * width : (h + 1) * width]
            return inner

        lax.fori_loop(b * bgroups, (b + 1) * bgroups, one_group, 0)
        for copy in out_copies[b]:
            copy.start()

    @pl.when(relay_here)
    def _():
        for b in range(blocks):
            wait(raw_out, hc * bgroups * mid, ret_ssem.at[b])

    for b in range(blocks):
        for copy in out_copies[b]:
            copy.wait()


def make(mesh):
    nrow, ncol = mesh.shape["row"], mesh.shape["col"]

    def on_device(density, green_octant):
        xl, width, extent = density.shape
        per = 128 // width
        groups = xl // per
        cells = xl * width
        hc = ncol // 2
        team = nrow * hc
        slots = extent // team
        each = min(max(EACH, 8 // groups), slots)
        chunks = slots // each
        blocks = min(BLOCKS, groups)
        mid = extent // 2
        k = np.arange(extent)[:, None]
        n = np.arange(extent)[None, :]
        theta = np.pi / (2 * extent) * (((2 * k + 1) * n) % (4 * extent))
        both = np.concatenate([np.cos(theta), np.sin(theta)], axis=0)
        shifted = np.pi / (4 * extent) * (((2 * k + 1) * (2 * n + 1 - extent)) % (8 * extent))
        waves = np.stack([np.cos(shifted), np.sin(shifted)])
        flip = np.eye(extent)[:, :mid]
        fold = np.stack([flip + flip[::-1], flip - flip[::-1]])
        tables = (
            halves(both.T),
            halves(both),
            halves(waves).transpose(1, 0, 2, 3),
            halves(waves.transpose(0, 2, 1)).transpose(1, 0, 2, 3),
            jnp.asarray(fold.astype(np.float32).astype(BF16)),
        )
        operands = (
            density.reshape(cells, extent),
            green_octant.reshape(cells, extent),
        ) + tables
        sizes = (nrow, ncol, groups, per, width, each, blocks)
        lot = extent * groups
        dma = pltpu.SemaphoreType.DMA
        any_space = pl.BlockSpec(memory_space=pl.ANY)
        out = pl.pallas_call(
            lambda *refs: fused_kernel(sizes, *refs),
            in_specs=[any_space] * len(operands),
            out_specs=any_space,
            out_shape=jax.ShapeDtypeStruct((cells, extent), F32),
            scratch_shapes=[pltpu.VMEM(v.shape, v.dtype) for v in operands]
            + [
                pltpu.VMEM((cells, extent), F32),
                pltpu.VMEM((2, cells, extent), BF16),
                pltpu.VMEM((2, cells, extent), BF16),
                pltpu.VMEM((cells, mid), F32),
                pltpu.VMEM((hc, cells, mid), F32),
                pltpu.VMEM(((1 + hc) * lot, 128), F32),
                pltpu.VMEM((2 * lot, 128), F32),
                pltpu.VMEM((lot, 128), F32),
                pltpu.VMEM((2 * lot, 128), F32),
                pltpu.VMEM((2 * lot, 128), F32),
                pltpu.VMEM(((1 + hc) * lot, 128), F32),
                pltpu.VMEM((hc, groups * mid, 128), F32),
                pltpu.VMEM((groups * mid, 128), F32),
                pltpu.VMEM((groups * extent, 128), F32),
                dma((6,)),
                dma((blocks, per)),
                dma((blocks, per)),
                dma((blocks,)),
                dma((hc, blocks)),
            ]
            + [dma((chunks,))] * 6
            + [dma((blocks,))] * 2
            + [dma((1,))] * 2
            + [dma((chunks,))],
            compiler_params=pltpu.CompilerParams(
                vmem_limit_bytes=VMEM_BYTES, collective_id=0, has_side_effects=True
            ),
            name="fused",
        )(*operands)
        return out.reshape(xl, width, extent)

    return on_device


EACH = 1
BLOCKS = 8
LEAD = 4


def solution(mesh):
    return jax.shard_map(
        make(mesh),
        mesh=mesh,
        in_specs=(P("row", "col", None), P("row", "col", None)),
        out_specs=P("row", "col", None),
        check_vma=False,
    )
```
